256 devices in a mesh: kgrp: 2 (over y), band: 16 (over z), fft: 8 (over x, core).
Axes of the slice: x: 4, y: 2, z: 16, core: 2. Of those that a mesh axis runs over, the one named last changes fastest.
The devices are a block of a 4x16x16 slice.
Arguments:
- orbitals: float32 [32, 64, 64, 128], P(('kgrp', 'band'), 'fft'), parts along dimension 0, may hold values from -6 to 6
- partners: float32 [32, 64, 64, 128], P(('kgrp', 'band'), 'fft'), parts along dimension 0, may hold values from -6 to 6
- shift_table: float32 [8, 3], replicated, may hold values from -0.5 to 0.5
- shift_index: int32 [32], P('kgrp'), parts along dimension 0, may hold values from 0 to 7
Outputs:
- potential: float32 [32, 64, 64, 128], P(('kgrp', 'band'), 'fft'), parts along dimension 0
- projector: float32 [32, 64, 64, 128], P(('kgrp', 'band'), 'fft'), parts along dimension 0
The draws below stay inside these ranges and needn't reach their ends.
There are 2 independent parts, one for each index of `kgrp`. The reference program is written for one: setup_inputs(seed, part) draws one part's arguments, and reference() takes and returns one part's arrays. A program takes and returns all parts, laid end to end along the dimension named above; an argument that names none is the same for every part. Nothing has to cross between parts.
All inputs are finite; a program needn't handle non-finite values.
Results may differ from the reference program's by a relative error of at most 0.0001.
Values sent between devices are 32-bit elements; how exact they have to be, the bound alone decides.
A program may use at most 64 MiB of HBM per device.

```python
import math
import jax
import jax.numpy as jnp
from jax import lax

GRID = 64
NQ = 8
BANDS = 16
PARTNERS = 16


def touch_ends(drawn, rng, least, top_value):
    longest = drawn.shape.index(max(drawn.shape))
    spots = []
    for shift in (0, 1):
        where = [jax.random.randint(jax.random.fold_in(rng, axis), (), 0, length) for axis, length in enumerate(drawn.shape)]
        where[longest] = (where[longest] + shift) % drawn.shape[longest]
        spots.append(tuple(where))
    return drawn.at[spots[0]].set(least).at[spots[1]].set(top_value)


def block_levels(stream_key, dims, pieces, low, high):
    loudness = 1.0
    for dim, parts in pieces:
        heights = jax.random.uniform(jax.random.fold_in(jax.random.fold_in(stream_key, 6), dim), (parts,), jnp.float32, low / len(pieces), high / len(pieces))
        loudness = loudness * jnp.repeat(jnp.exp(heights), dims[dim] // parts).reshape((-1,) + (1,) * (len(dims) - 1 - dim))
    return loudness


def noise(stream_key, shape, scale, bound, split=(), kind=jnp.bfloat16):
    result = jax.random.normal(stream_key, shape, jnp.float32) * scale
    if len(split) > 0:
        result = block_levels(stream_key, shape, split, -0.22, 0.18) * result
    return jnp.clip(result, min=-bound, max=bound).astype(kind)


def setup_inputs(seed: int = 0, part: int = 0) -> dict:
    arg_keys = jax.random.split(jax.random.key(seed), 5)
    part_keys = jax.random.split(jax.random.fold_in(arg_keys[4], part), 5)
    orbitals = noise(part_keys[0], (BANDS, GRID, GRID, 2 * GRID), 0.7, 6.0, ((0, 16), (1, 8)), jnp.float32)
    partners = noise(part_keys[1], (PARTNERS, GRID, GRID, 2 * GRID), 0.7, 6.0, ((0, 16), (1, 8)), jnp.float32)
    shift_table = jnp.clip(jax.random.uniform(arg_keys[2], (NQ, 3), jnp.float32, -0.5, 0.5), -0.5, 0.5)
    shift_index = touch_ends(jax.random.randint(part_keys[3], (PARTNERS,), 0, NQ), jax.random.fold_in(part_keys[3], 1), 0, NQ - 1).astype(jnp.int32)
    return {"orbitals": orbitals, "partners": partners, "shift_table": shift_table, "shift_index": shift_index}


HIGHEST = lax.Precision.HIGHEST
SCREEN_SQUARE = 0.25
FOUR_PI = 4.0 * math.pi

def frequency(positions, extent):
    return jnp.where(positions < extent // 2, positions, positions - extent).astype(jnp.float32)

def rotate(field):
    extent = field.shape[-1] // 2
    return jnp.concatenate([field[..., extent:], -field[..., :extent]], axis=-1)

def factor_inverse(over_real, over_imag):
    matrix_order = over_real.shape[0]
    positions = jnp.arange(matrix_order, dtype=jnp.int32)
    zero_start = jnp.zeros_like(over_real)

    def chol_step(column, lowers):
        lower_real, lower_imag = lowers
        row_real = lower_real[column]
        row_imag = lower_imag[column]
        resid_real = over_real[:, column] - (jnp.dot(lower_real, row_real, precision=HIGHEST) + jnp.dot(lower_imag, row_imag, precision=HIGHEST))
        resid_imag = over_imag[:, column] - (jnp.dot(lower_imag, row_real, precision=HIGHEST) - jnp.dot(lower_real, row_imag, precision=HIGHEST))
        pivot_value = jnp.sqrt(resid_real[column])
        below_diag = positions > column
        at_diag = positions == column
        new_real = jnp.where(below_diag, resid_real / pivot_value, jnp.where(at_diag, pivot_value, 0.0))
        new_imag = jnp.where(below_diag, resid_imag / pivot_value, 0.0)
        chosen = positions[None, :] == column
        return (jnp.where(chosen, new_real[:, None], lower_real), jnp.where(chosen, new_imag[:, None], lower_imag))
    lower_real, lower_imag = lax.fori_loop(0, matrix_order, chol_step, (zero_start, zero_start))

    def solve_step(row_index, inverses):
        inv_real, inv_imag = inverses
        row_real = lower_real[row_index]
        row_imag = lower_imag[row_index]
        sum_real = jnp.dot(row_real, inv_real, precision=HIGHEST) - jnp.dot(row_imag, inv_imag, precision=HIGHEST)
        sum_imag = jnp.dot(row_real, inv_imag, precision=HIGHEST) + jnp.dot(row_imag, inv_real, precision=HIGHEST)
        unit_row = (positions == row_index).astype(over_real.dtype)
        pivot_value = lower_real[row_index, row_index]
        new_real = (unit_row - sum_real) / pivot_value
        new_imag = -sum_imag / pivot_value
        chosen = positions[:, None] == row_index
        return (jnp.where(chosen, new_real[None, :], inv_real), jnp.where(chosen, new_imag[None, :], inv_imag))
    return lax.fori_loop(0, matrix_order, solve_step, (zero_start, zero_start))

def reference(orbitals, partners, shift_table, shift_index):
    extent = orbitals.shape[1]
    orbital_field = orbitals[..., :extent] + 1j * orbitals[..., extent:]
    partner_field = partners[..., :extent] + 1j * partners[..., extent:]
    grid_freq = frequency(jnp.arange(extent, dtype=jnp.int32), extent).astype(orbitals.dtype)

    def partner_term(running, member):
        single, chosen_index = member
        qvector = shift_table[chosen_index]
        denominator = (grid_freq[:, None, None] + qvector[0]) ** 2 + (grid_freq[None, :, None] + qvector[1]) ** 2 + (grid_freq[None, None, :] + qvector[2]) ** 2 + SCREEN_SQUARE
        kernel = FOUR_PI / denominator
        density = jnp.conj(single)[None] * orbital_field
        field = jnp.fft.ifftn(jnp.fft.fftn(density, axes=(1, 2, 3)) * kernel[None], axes=(1, 2, 3))
        return (running + single[None] * field, None)
    start_field = jnp.zeros(orbital_field.shape, orbital_field.dtype)
    exchange_field, _ = lax.scan(partner_term, start_field, (partner_field, shift_index))
    potential = jnp.concatenate([exchange_field.real, exchange_field.imag], axis=-1).astype(orbitals.dtype)
    total_bands = potential.shape[0]
    turned = rotate(potential)
    flat_orbitals = orbitals.reshape(total_bands, -1)
    flat_pot = potential.reshape(total_bands, -1)
    flat_turned = turned.reshape(total_bands, -1)
    volume = float(extent ** 3)
    over_real = jnp.einsum('ik,jk->ij', flat_orbitals, flat_pot, precision=HIGHEST) / volume
    over_imag = jnp.einsum('ik,jk->ij', flat_orbitals, flat_turned, precision=HIGHEST) / volume
    inv_real, inv_imag = factor_inverse(over_real, over_imag)
    projector = jnp.dot(inv_real, flat_pot, precision=HIGHEST) + jnp.dot(inv_imag, flat_turned, precision=HIGHEST)
    return (potential, projector.reshape(potential.shape))
```

```python
import math

import jax
import jax.numpy as jnp
import numpy as np
from jax import lax
from jax.experimental import pallas as pl
from jax.experimental.pallas import tpu as pltpu
from jax.sharding import PartitionSpec as P

SCREEN_SQUARE = 0.25
FOUR_PI = 4.0 * math.pi
MESH = pl.DeviceIdType.MESH
PAD = 8
BF = jnp.bfloat16
F32 = jnp.float32


def split_table(table):
    high = np.asarray(table, np.float64).astype(jnp.bfloat16)
    low = (np.asarray(table, np.float64) - high.astype(np.float64)).astype(jnp.bfloat16)
    return high, low


def dft(extent):
    k = np.arange(extent)
    angle = 2.0 * np.pi * ((k[:, None] * k[None, :]) % extent) / extent
    return np.cos(angle), np.sin(angle)


def last_table(extent, sign):
    cosine, sine = dft(extent)
    sine = sign * sine
    table = np.block([[cosine, sine], [-sine, cosine]])
    high, low = split_table(table)
    both = np.concatenate([high, low], axis=1)
    return np.concatenate([both, both], axis=0)


def left_table(extent, sign):
    cosine, sine = dft(extent)
    table = np.concatenate([cosine, -sign * sine], axis=1)
    high, low = split_table(table)
    return np.concatenate(
        [np.concatenate([high, high], axis=1), np.concatenate([low, low], axis=1)], axis=0
    )


def halves(v):
    high = v.astype(BF)
    low = (v - high.astype(F32)).astype(BF)
    return high, low


def swapped(v):
    return pltpu.roll(v, v.shape[-1] // 2, 1)


def lane_sign(shape, first, second):
    lane = lax.broadcasted_iota(jnp.int32, shape, len(shape) - 1)
    return jnp.where(lane < shape[-1] // 2, first, second).astype(F32)


def turned(v):
    return swapped(v) * lane_sign((1, v.shape[-1]), 1.0, -1.0)


def mm(a, b):
    return jnp.dot(a, b, preferred_element_type=F32)


def along_last(v, table):
    high, low = halves(v)
    width = v.shape[-1]
    both = mm(jnp.concatenate([high, low], axis=1), table)
    return both[:, :width] + both[:, width:]


def left_column(v):
    high, low = halves(v)
    thigh, tlow = halves(turned(v))
    return jnp.concatenate([high, thigh, low, tlow], axis=0)


def along_left(blocks, table):
    rows = table.shape[0] // 2
    columns = jnp.concatenate([left_column(v) for v in blocks], axis=1)
    both = mm(table, columns)
    out = both[:rows] + both[rows:]
    width = blocks[0].shape[-1]
    return [out[:, k * width : (k + 1) * width] for k in range(len(blocks))]


def kernel(
    nb, nf, n, p_hbm, u_hbm, zf_ref, zi_ref, lf_ref, li_ref, tab_ref, idx_ref,
    pot_ref, proj_ref,
    pfull, ufull, dbuf, vbuf, d2d, hops, usub, vsub, psub, mine, mrow, mcol, mall,
    perm_s, perm_r, loc, agz_s, agz_r, agx_s, agx_r, du_s, du_r, dv_s, dv_r, rs_s, rs_r,
    au_s, au_r, av_s, av_r, ap_s, ap_r, mf_s, mf_r, mb_s, mb_r,
):
    slab = p_hbm.shape[0]
    half = slab // 2
    planes = slab // n
    width = p_hbm.shape[1]
    nx = nf // 2
    part = slab // nb
    pitch = n + PAD
    b = lax.axis_index("band")
    f = lax.axis_index("fft")
    x, c = f // 2, f % 2
    mate = f + 1 - 2 * c
    right, left = (b + 1) % nb, (b + nb - 1) % nb
    fright, fleft = (f + 2) % nf, (f + nf - 2) % nf
    slot = (b - f + nf // 2 + nb) % nb
    to_band, to_fft, to_slot = (b - nf // 2 + f + nb) % nb, b % nf, (b // nf) * nf + f
    from_band, from_fft = f + nf * (slot // nf), slot % nf
    alone = jnp.logical_and(to_band == b, to_fft == f)

    def rows(start, count):
        return pl.ds(pl.multiple_of(start, 8), count)

    def rc(src, dst, ssem, rsem, **dev):
        return pltpu.make_async_remote_copy(
            src_ref=src, dst_ref=dst, send_sem=ssem, recv_sem=rsem, device_id=dev,
            device_id_type=MESH,
        )

    barrier = pltpu.get_barrier_semaphore()

    def greet(**dev):
        pl.semaphore_signal(barrier, inc=1, device_id=dev, device_id_type=MESH)

    @pl.loop(1, nb)
    def _(d):
        greet(band=(b + d) % nb)

    @pl.loop(1, nf)
    def _(d):
        greet(fft=(f + d) % nf)

    @pl.when(jnp.logical_not(alone))
    def _():
        greet(band=to_band, fft=to_fft)
        greet(band=from_band, fft=from_fft)

    u_local = pltpu.make_async_copy(u_hbm, ufull.at[rows(f * slab, slab)], loc.at[0])
    u_local.start()
    pl.semaphore_wait(barrier, nb - 1 + nf - 1 + jnp.where(alone, 0, 2))

    def perm(h):
        return rc(
            p_hbm.at[rows(h * half, half)], pfull.at[rows(to_slot * slab + h * half, half)],
            perm_s.at[h], perm_r.at[h], band=to_band, fft=to_fft,
        )

    def perm_here(h):
        return rc(
            p_hbm.at[rows(h * half, half)], pfull.at[rows(slot * slab + h * half, half)],
            perm_s.at[h], perm_r.at[h], band=from_band, fft=from_fft,
        )

    def perm_local(h):
        return pltpu.make_async_copy(
            p_hbm.at[rows(h * half, half)], pfull.at[rows(slot * slab + h * half, half)],
            loc.at[1 + h],
        )

    @pl.when(jnp.logical_not(alone))
    def _():
        perm(0).start()
        perm(1).start()

    @pl.when(alone)
    def _():
        perm_local(0).start()
        perm_local(1).start()

    def slab_of(dx, core):
        return 2 * ((x + dx) % nx) + core

    def agx1(h, way):
        return rc(
            u_hbm.at[rows(h * half, half)], ufull.at[rows(f * slab + h * half, half)],
            agx_s.at[0, h, way], agx_r.at[0, h, way], fft=fright if way == 0 else fleft,
        )

    def agx1_here(h, way):
        owner = slab_of(nx - 1 if way == 0 else 1, c)
        return rc(
            u_hbm.at[rows(h * half, half)], ufull.at[rows(owner * slab + h * half, half)],
            agx_s.at[0, h, way], agx_r.at[0, h, way], fft=fright if way == 0 else fleft,
        )

    def agx2(way):
        owner = slab_of(nx - 1 if way == 0 else 1, c)
        piece = ufull.at[rows(owner * slab + way * half, half)]
        return rc(
            piece, piece, agx_s.at[1, 0, way], agx_r.at[1, 0, way],
            fft=fright if way == 0 else fleft,
        )

    def agx2_here(way):
        piece = ufull.at[rows(slab_of(2, c) * slab + way * half, half)]
        return rc(
            piece, piece, agx_s.at[1, 0, way], agx_r.at[1, 0, way],
            fft=fright if way == 0 else fleft,
        )

    def du(k, core):
        piece = ufull.at[rows(slab_of((0, nx - 1, 1, 2)[k], core) * slab, slab)]
        src = u_hbm if (k == 0) else piece
        return rc(src, piece, du_s.at[k], du_r.at[k], fft=mate)

    for way in (0, 1):
        agx1(way, way).start()
    for way in (0, 1):
        agx1(1 - way, way).start()
    du(0, c).start()

    def agz(s, h, way):
        owner = (slot - (s - 1) + nb) % nb if way == 0 else (slot + (s - 1)) % nb
        piece = pfull.at[rows(owner * slab + h * half, half)]
        return rc(
            piece, piece, agz_s.at[s, h, way], agz_r.at[s, h, way],
            band=right if way == 0 else left,
        )

    def agz_here(s, h, way):
        owner = (slot - s + nb) % nb if way == 0 else (slot + s) % nb
        piece = pfull.at[rows(owner * slab + h * half, half)]
        return rc(
            piece, piece, agz_s.at[s, h, way], agz_r.at[s, h, way],
            band=right if way == 0 else left,
        )

    for h in (0, 1):
        @pl.when(jnp.logical_not(alone))
        def _():
            perm_here(h).wait_recv()

        @pl.when(alone)
        def _():
            perm_local(h).wait()

        for way in (0, 1):
            agz(1, h, way).start()

    for way in (0, 1):
        agx1_here(way, way).wait_recv()
        agx2(way).start()
    for way in (0, 1):
        agx1_here(1 - way, way).wait_recv()
        du(1 + way, c).start()

    for h in (0, 1):
        for way in (0, 1):
            agz_here(1, h, way).wait_recv()
            agz(2, h, way).start()

    for way in (0, 1):
        agx2_here(way).wait_recv()
    du(3, c).start()
    u_local.wait()
    for k in range(4):
        du(k, 1 - c).wait_recv()

    first_lanes = lax.broadcasted_iota(jnp.int32, (1, width), 1) < width // 2
    batch = 4

    def forward_planes(owner, k):
        a, s = owner // nf, owner % nf
        p = pfull[rows(owner * slab + k * batch * n, batch * n), :]
        u = ufull[rows(s * slab + k * batch * n, batch * n), :]
        ps, us = swapped(p), swapped(u)
        real = jnp.where(first_lanes, p, ps)
        imag = jnp.where(first_lanes, ps, -p)
        rho = real * u + imag * us
        spec = along_last(rho, zf_ref[...])
        base = (a * n + s * planes + k * batch) * pitch
        for q in range(0, batch, 2):
            outs = along_left(
                [spec[q * n : (q + 1) * n], spec[(q + 1) * n : (q + 2) * n]], lf_ref[...]
            )
            for e in (0, 1):
                dbuf[rows(base + (q + e) * pitch, n), :] = outs[e]

    last = nb // 2

    @pl.loop(3, last + 3)
    def _(s):
        @pl.when(s < last)
        def _():
            for h in (0, 1):
                for way in (0, 1):
                    agz_here(s - 1, h, way).wait_recv()
                    agz(s, h, way).start()

        @pl.when(s == last)
        def _():
            for h in (0, 1):
                for way in (0, 1):
                    agz_here(s - 1, h, way).wait_recv()
                    if h == way:
                        agz(s, h, way).start()

        @pl.when(s == last + 1)
        def _():
            for way in (0, 1):
                agz_here(last, way, way).wait_recv()

        end = s == last + 2
        low = (slot - jnp.where(end, 0, s - 2) + nb) % nb
        high = (slot + jnp.where(end, last, s - 2)) % nb

        @pl.loop(0, 2 * (planes // batch))
        def _(k):
            owner = jnp.where(k < planes // batch, low, high)
            forward_planes(owner, k % (planes // batch))

    def a2a(src_of, dst, ssem, rsem, d):
        to = (b + d) % nb
        return rc(src_of(to), dst.at[rows(b * part, part)], ssem.at[d], rsem.at[d], band=to)

    def a2a_here(src_of, dst, ssem, rsem, d):
        to = (b + d) % nb
        source = (b - d + nb) % nb
        return rc(src_of(to), dst.at[rows(source * part, part)], ssem.at[d], rsem.at[d], band=to)

    au = (lambda t: u_hbm.at[rows(t * part, part)], usub, au_s, au_r)

    @pl.loop(1, nb)
    def _(d):
        a2a(*au, d).start()

    u_mine = pltpu.make_async_copy(
        u_hbm.at[rows(b * part, part)], usub.at[rows(b * part, part)], loc.at[3]
    )
    u_mine.start()

    freq = lax.broadcasted_iota(jnp.int32, (n, width), 0)
    freq = jnp.where(freq < n // 2, freq, freq - n).astype(F32)
    lane = lax.broadcasted_iota(jnp.int32, (n, width), 1) % n
    lane = jnp.where(lane < n // 2, lane, lane - n).astype(F32)
    shift = []
    for a in (0, 1):
        row = idx_ref[f + nf * a]
        shift.append([tab_ref[row, e] for e in range(3)])
    for a in (0, 1):
        fx = freq + shift[a][0]
        fz = lane + shift[a][2]
        hops[rows(a * n, n), :] = fx * fx + fz * fz + SCREEN_SQUARE
    scale = FOUR_PI / n**3
    per = 2

    @pl.loop(0, n // per)
    def _(k):
        for a in (0, 1):
            ys = [k * per + e for e in range(per)]
            take = [pl.ds(a * n * pitch + y, n, stride=pitch) for y in ys]
            spectra = along_left([dbuf[t, :] for t in take], lf_ref[...])
            base = hops[pl.ds(a * n, n), :]
            screened = []
            for y, spectrum in zip(ys, spectra):
                fy = jnp.where(y < n // 2, y, y - n).astype(F32) + shift[a][1]
                screened.append(spectrum * (scale / (base + fy * fy)))
            fields = along_left(screened, li_ref[...])
            for t, field in zip(take, fields):
                dbuf[t, :] = field

    def dv(k):
        src = vbuf.at[rows(slab_at(k, 1 - c) * slab, slab)]
        return rc(src, d2d.at[rows(k * slab, slab)], dv_s.at[k], dv_r.at[k], fft=mate)

    def slab_at(k, core):
        dx = jnp.where(k == 0, 2, jnp.where(k == 1, 1, jnp.where(k == 2, nx - 1, 0)))
        return slab_of(dx, core)

    def hop(k, src, way):
        return rc(
            src, hops.at[rows(2 * n + k * half, half)], rs_s.at[k], rs_r.at[k],
            fft=fright if way == 0 else fleft,
        )

    def piece(dx, h):
        return vbuf.at[rows(slab_of(dx, c) * slab + h * half, half)]

    def hop_of(k):
        way = k % 2
        toward = 1 if way == 0 else nx - 1
        if k < 2:
            return hop(k, piece(2, way), way)
        if k < 4:
            return hop(k, piece(toward, 1 - way), way)
        return hop(k, piece(toward, way), way)

    def inverse_planes(s, k):
        total = None
        for a in (0, 1):
            base = (a * n + s * planes + k * batch) * pitch
            fields = []
            for q in range(0, batch, 2):
                fields += along_left(
                    [dbuf[rows(base + (q + e) * pitch, n), :] for e in (0, 1)], li_ref[...]
                )
            field = along_last(jnp.concatenate(fields, axis=0), zi_ref[...])
            p = pfull[rows((a * nf + s) * slab + k * batch * n, batch * n), :]
            ps = swapped(p)
            real = jnp.where(first_lanes, p, ps)
            imag = jnp.where(first_lanes, -ps, p)
            term = real * field + imag * swapped(field)
            total = term if total is None else total + term
        vbuf[rows(s * slab + k * batch * n, batch * n), :] = total

    @pl.loop(0, 2 * nx)
    def _(i):
        own = i >= nx
        k = i % nx
        s = slab_at(k, jnp.where(own, c, 1 - c))

        @pl.loop(0, planes // batch)
        def _(q):
            inverse_planes(s, q)

        @pl.when(jnp.logical_not(own))
        def _():
            dv(k).start()

        @pl.when(own)
        def _():
            dv(k).wait_recv()
            vbuf[rows(s * slab, slab), :] += d2d[rows(k * slab, slab), :]

        @pl.when(i == nx)
        def _():
            hop_of(0).start()
            hop_of(1).start()

        @pl.when(i == nx + 1)
        def _():
            hop_of(2).start()

        @pl.when(i == nx + 2)
        def _():
            hop_of(3).start()

    def arrived(k):
        return hops[rows(2 * n + k * half, half), :]

    for way in (0, 1):
        hop_of(way).wait_recv()
        toward = slab_of(1 if way == 0 else nx - 1, c)
        vbuf[rows(toward * slab + way * half, half), :] += arrived(way)
        hop_of(4 + way).start()
    for k in (2, 3, 4, 5):
        hop_of(k).wait_recv()
    pot_ref[0:half, :] = vbuf[rows(f * slab, half), :] + arrived(3) + arrived(4)
    pot_ref[half:slab, :] = vbuf[rows(f * slab + half, half), :] + arrived(2) + arrived(5)

    av = (lambda t: pot_ref.at[rows(t * part, part)], vsub, av_s, av_r)

    @pl.loop(1, nb)
    def _(d):
        a2a(*av, d).start()

    vsub[rows(b * part, part), :] = pot_ref[rows(b * part, part), :]
    u_mine.wait()

    @pl.loop(1, nb)
    def _(d):
        a2a_here(*au, d).wait_recv()

    @pl.loop(1, nb)
    def _(d):
        a2a_here(*av, d).wait_recv()

    group = 4
    acc = jnp.zeros((2 * nb, 4 * nb), F32)
    for g in range(0, part, group):
        us = [usub[pl.ds(g + e, nb, stride=part), :] for e in range(group)]
        vs = [vsub[pl.ds(g + e, nb, stride=part), :] for e in range(group)]
        uh, ul = halves(jnp.concatenate(us, axis=1))
        vh, vl = halves(jnp.concatenate(vs, axis=1))
        th, tl = halves(jnp.concatenate([turned(v) for v in vs], axis=1))
        acc += lax.dot_general(
            jnp.concatenate([uh, ul], axis=0), jnp.concatenate([vh, th, vl, tl], axis=0),
            (((1,), (1,)), ((), ())), preferred_element_type=F32,
        )
    acc = acc[:nb] + acc[nb:]
    acc = (acc[:, : 2 * nb] + acc[:, 2 * nb :]) * (1.0 / n**3)
    mine[...] = jnp.concatenate([acc, jnp.zeros((nb, width - 2 * nb), F32)], axis=1)

    def mf(d, here=False):
        to = (f + d) % nf
        source = (f - d + nf) % nf
        at = source if here else f
        return rc(mine, mrow.at[rows(at * nb, nb)], mf_s.at[d], mf_r.at[d], fft=to)

    def mb(d, here=False):
        to = (b + d) % nb
        source = (b - d + nb) % nb
        at = source if here else b
        return rc(mcol, mall.at[rows(at * nb, nb)], mb_s.at[d], mb_r.at[d], band=to)

    for d in range(1, nf):
        mf(d).start()
    mrow[rows(f * nb, nb), :] = mine[...]
    for d in range(1, nf):
        mf(d, True).wait_recv()
    total = mrow[0:nb, :]
    for k in range(1, nf):
        total += mrow[k * nb : (k + 1) * nb, :]
    mcol[...] = total

    @pl.loop(1, nb)
    def _(d):
        mb(d).start()

    mall[rows(b * nb, nb), :] = mcol[...]

    @pl.loop(1, nb)
    def _(d):
        mb(d, True).wait_recv()

    total = mall[0:nb, :]
    for k in range(1, nb):
        total += mall[k * nb : (k + 1) * nb, :]

    ri = lax.broadcasted_iota(jnp.int32, (nb, nb), 0)
    ci = lax.broadcasted_iota(jnp.int32, (nb, nb), 1)
    eye = (ri == ci).astype(F32)

    def flipped(m):
        return lax.dot_general(
            eye, m, (((1,), (1,)), ((), ())), precision=lax.Precision.HIGHEST,
            preferred_element_type=F32,
        )

    mre, mim = total[:, :nb], total[:, nb : 2 * nb]
    hre = jnp.where(ri >= ci, mre, flipped(mre))
    him = jnp.where(ri > ci, mim, jnp.where(ri < ci, -flipped(mim), 0.0))
    zero = jnp.zeros((nb, nb), F32)
    work = jnp.concatenate([hre, him, eye, zero], axis=1)
    other = jnp.concatenate([-him, hre, zero, eye], axis=1)
    row_at = lax.broadcasted_iota(jnp.int32, (nb, 1), 0)
    for k in range(nb):
        pivot = work[k : k + 1, k : k + 1]
        cre = jnp.where(row_at > k, work[:, k : k + 1], 0.0) / pivot
        cim = jnp.where(row_at > k, work[:, nb + k : nb + k + 1], 0.0) / pivot
        row, rot = work[k : k + 1, :], other[k : k + 1, :]
        work = work - (cre * row + cim * rot)
        other = other - (cre * rot - cim * row)
    pivots = jnp.sum(work[:, :nb] * eye, axis=1, keepdims=True)
    coef = work[:, 2 * nb : 4 * nb] / jnp.sqrt(pivots)
    ch, cl = halves(coef)
    coef = jnp.concatenate(
        [jnp.concatenate([ch, ch], axis=1), jnp.concatenate([cl, cl], axis=1)], axis=0
    )

    for g in range(0, part, group):
        vs = [vsub[pl.ds(g + e, nb, stride=part), :] for e in range(group)]
        cols = jnp.concatenate([left_column(v) for v in vs], axis=1)
        both = mm(coef, cols)
        out = both[:nb] + both[nb:]
        for e in range(group):
            psub[pl.ds(g + e, nb, stride=part), :] = out[:, e * width : (e + 1) * width]

    ap = (lambda t: psub.at[rows(t * part, part)], proj_ref, ap_s, ap_r)

    @pl.loop(1, nb)
    def _(d):
        a2a(*ap, d).start()

    proj_ref[rows(b * part, part), :] = psub[rows(b * part, part), :]

    @pl.when(jnp.logical_not(alone))
    def _():
        perm(0).wait_send()
        perm(1).wait_send()

    for way in (0, 1):
        for h in (0, 1):
            agx1(h, way).wait_send()
        agx2(way).wait_send()
    for k in range(4):
        du(k, c).wait_send()

    @pl.loop(1, last)
    def _(s):
        for h in (0, 1):
            for way in (0, 1):
                agz(s, h, way).wait_send()

    for way in (0, 1):
        agz(last, way, way).wait_send()

    @pl.loop(0, nx)
    def _(k):
        dv(k).wait_send()

    for k in range(6):
        hop_of(k).wait_send()
    for d in range(1, nf):
        mf(d).wait_send()

    @pl.loop(1, nb)
    def _(d):
        a2a(*au, d).wait_send()
        a2a(*av, d).wait_send()
        mb(d).wait_send()
        a2a(*ap, d).wait_send()

    @pl.loop(1, nb)
    def _(d):
        a2a_here(*ap, d).wait_recv()


def body(mesh, orbitals, partners, shift_table, shift_index):
    nb, nf = mesh.shape["band"], mesh.shape["fft"]
    n = orbitals.shape[2]
    width = orbitals.shape[3]
    slab = orbitals.shape[0] * orbitals.shape[1] * n
    part = slab // nb
    assert nb == 2 * nf and nf == 8 and orbitals.shape[0] == 1

    def call(p, u, *rest):
        any_spec = pl.BlockSpec(memory_space=pl.ANY)
        vmem = pl.BlockSpec(memory_space=pltpu.VMEM)
        smem = pl.BlockSpec(memory_space=pltpu.SMEM)
        dma = pltpu.SemaphoreType.DMA
        out = jax.ShapeDtypeStruct((slab, width), F32)
        half = slab // 2
        return pl.pallas_call(
            lambda *refs: kernel(nb, nf, n, *refs),
            out_shape=(out, out),
            in_specs=[any_spec, any_spec, vmem, vmem, vmem, vmem, smem, smem],
            out_specs=(vmem, vmem),
            scratch_shapes=[
                pltpu.VMEM((nb * slab, width), F32),
                pltpu.VMEM((nf * slab, width), F32),
                pltpu.VMEM((2 * n * (n + PAD), width), F32),
                pltpu.VMEM((nf * slab, width), F32),
                pltpu.VMEM((nf // 2 * slab, width), F32),
                pltpu.VMEM((2 * n + 6 * half, width), F32),
                pltpu.VMEM((slab, width), F32),
                pltpu.VMEM((slab, width), F32),
                pltpu.VMEM((slab, width), F32),
                pltpu.VMEM((nb, width), F32),
                pltpu.VMEM((nf * nb, width), F32),
                pltpu.VMEM((nb, width), F32),
                pltpu.VMEM((nb * nb, width), F32),
                dma((2,)), dma((2,)), dma((4,)),
                dma((nb // 2 + 1, 2, 2)), dma((nb // 2 + 1, 2, 2)),
                dma((2, 2, 2)), dma((2, 2, 2)),
                dma((4,)), dma((4,)), dma((4,)), dma((4,)), dma((6,)), dma((6,)),
                dma((nb,)), dma((nb,)), dma((nb,)), dma((nb,)), dma((nb,)), dma((nb,)),
                dma((nf,)), dma((nf,)), dma((nb,)), dma((nb,)),
            ],
            compiler_params=pltpu.CompilerParams(collective_id=0, has_side_effects=True),
            name="exchange",
        )(p, u, *rest)

    tables = [
        jnp.asarray(t)
        for t in (last_table(n, -1.0), last_table(n, 1.0), left_table(n, -1.0), left_table(n, 1.0))
    ]
    pot, proj = call(
        partners.reshape(slab, width), orbitals.reshape(slab, width), *tables,
        shift_table, shift_index,
    )
    return pot.reshape(orbitals.shape), proj.reshape(orbitals.shape)


def solution(mesh):
    spec = P(("kgrp", "band"), "fft", None, None)
    return jax.shard_map(
        lambda *args: body(mesh, *args), mesh=mesh, in_specs=(spec, spec, P(), P("kgrp")),
        out_specs=(spec, spec), check_vma=False,
    )
```

```python
import math

import jax
import jax.numpy as jnp
import numpy as np
from jax import lax
from jax.experimental import pallas as pl
from jax.experimental.pallas import tpu as pltpu
from jax.sharding import PartitionSpec as P

SCREEN_SQUARE = 0.25
FOUR_PI = 4.0 * math.pi
MESH = pl.DeviceIdType.MESH
SPREAD = 5
PAD = 8
BF = jnp.bfloat16
F32 = jnp.float32


def split_table(table):
    high = np.asarray(table, np.float64).astype(jnp.bfloat16)
    low = (np.asarray(table, np.float64) - high.astype(np.float64)).astype(jnp.bfloat16)
    return high, low


def dft(extent):
    k = np.arange(extent)
    angle = 2.0 * np.pi * ((k[:, None] * k[None, :]) % extent) / extent
    return np.cos(angle), np.sin(angle)


def last_table(extent, sign):
    cosine, sine = dft(extent)
    sine = sign * sine
    table = np.block([[cosine, sine], [-sine, cosine]])
    high, low = split_table(table)
    both = np.concatenate([high, low], axis=1)
    return np.concatenate([both, both], axis=0)


def left_table(extent, sign):
    cosine, sine = dft(extent)
    table = np.concatenate([cosine, -sign * sine], axis=1)
    high, low = split_table(table)
    return np.concatenate(
        [np.concatenate([high, high], axis=1), np.concatenate([low, low], axis=1)], axis=0
    )


def halves(v):
    high = v.astype(BF)
    low = (v - high.astype(F32)).astype(BF)
    return high, low


def swapped(v):
    return pltpu.roll(v, v.shape[-1] // 2, 1)


def lane_sign(shape, first, second):
    lane = lax.broadcasted_iota(jnp.int32, shape, len(shape) - 1)
    return jnp.where(lane < shape[-1] // 2, first, second).astype(F32)


def turned(v):
    return swapped(v) * lane_sign((1, v.shape[-1]), 1.0, -1.0)


def mm(a, b):
    return jnp.dot(a, b, preferred_element_type=F32)


def along_last(v, table):
    high, low = halves(v)
    width = v.shape[-1]
    both = mm(jnp.concatenate([high, low], axis=1), table)
    return both[:, :width] + both[:, width:]


def left_column(v):
    high, low = halves(v)
    thigh, tlow = halves(turned(v))
    return jnp.concatenate([high, thigh, low, tlow], axis=0)


def along_left(blocks, table):
    rows = table.shape[0] // 2
    columns = jnp.concatenate([left_column(v) for v in blocks], axis=1)
    both = mm(table, columns)
    out = both[:rows] + both[rows:]
    width = blocks[0].shape[-1]
    return [out[:, k * width : (k + 1) * width] for k in range(len(blocks))]


def kernel(
    nb, nf, n, p_hbm, u_hbm, zf_ref, zi_ref, lf_ref, li_ref, tab_ref, idx_ref,
    pot_ref, proj_ref,
    pfull, ufull, dbuf, vbuf, d2d, hops, usub, vsub, psub, mine, mrow, mcol, mall,
    perm_s, perm_r, loc, agz_s, agz_r, agx_s, agx_r, du_s, du_r, dv_s, dv_r, rs_s, rs_r,
    au_s, au_r, av_s, av_r, ap_s, ap_r, mf_s, mf_r, mb_s, mb_r,
):
    slab = p_hbm.shape[0]
    half = slab // 2
    quarters = 4
    quarter = slab // quarters
    planes = slab // n
    width = p_hbm.shape[1]
    nx = nf // 2
    part = slab // nb
    pitch = n + PAD
    b = lax.axis_index("band")
    f = lax.axis_index("fft")
    x, c = f // 2, f % 2
    mate = f + 1 - 2 * c
    right, left = (b + 1) % nb, (b + nb - 1) % nb
    fright, fleft = (f + 2) % nf, (f + nf - 2) % nf
    lead = x + nx * c
    slot = (b - lead + nf // 2 + nb) % nb
    to_band = (b - nf // 2 + (SPREAD * f) % nf + nb) % nb
    to_fft = 2 * (b % nx) + (b // nx) % 2
    to_slot = (b // nf) * nf + f
    from_fft = (SPREAD * slot) % nf
    from_band = lead + nf * (slot // nf)
    alone = jnp.logical_and(to_band == b, to_fft == f)

    def farthest_first(i, count):
        return count // 2 + jnp.where(i % 2 == 0, i // 2, -(i // 2))

    def rows(start, count):
        return pl.ds(pl.multiple_of(start, 8), count)

    def rc(src, dst, ssem, rsem, **dev):
        return pltpu.make_async_remote_copy(
            src_ref=src, dst_ref=dst, send_sem=ssem, recv_sem=rsem, device_id=dev,
            device_id_type=MESH,
        )

    barrier = pltpu.get_barrier_semaphore()

    def greet(**dev):
        pl.semaphore_signal(barrier, inc=1, device_id=dev, device_id_type=MESH)

    greet(band=right)
    greet(band=left)
    greet(fft=fright)
    greet(fft=fleft)
    greet(fft=mate)

    @pl.when(jnp.logical_not(alone))
    def _():
        greet(band=to_band, fft=to_fft)
        greet(band=from_band, fft=from_fft)

    u_local = pltpu.make_async_copy(u_hbm, ufull.at[rows(f * slab, slab)], loc.at[0])
    u_local.start()
    pl.semaphore_wait(barrier, jnp.where(alone, 5, 7))

    def place(at):
        return (at // nf) * nf + (SPREAD * at) % nf

    def perm(q):
        return rc(
            p_hbm.at[rows(q * quarter, quarter)],
            pfull.at[rows(to_slot * slab + q * quarter, quarter)],
            perm_s.at[q], perm_r.at[q], band=to_band, fft=to_fft,
        )

    def perm_here(q):
        return rc(
            p_hbm.at[rows(q * quarter, quarter)],
            pfull.at[rows(place(slot) * slab + q * quarter, quarter)],
            perm_s.at[q], perm_r.at[q], band=from_band, fft=from_fft,
        )

    def perm_local(q):
        return pltpu.make_async_copy(
            p_hbm.at[rows(q * quarter, quarter)],
            pfull.at[rows(place(slot) * slab + q * quarter, quarter)], loc.at[2 + q],
        )

    @pl.when(jnp.logical_not(alone))
    def _():
        for q in range(quarters):
            perm(q).start()

    @pl.when(alone)
    def _():
        for q in range(quarters):
            perm_local(q).start()

    def slab_of(dx, core):
        return 2 * ((x + dx) % nx) + core

    def agx1(h, way):
        return rc(
            u_hbm.at[rows(h * half, half)], ufull.at[rows(f * slab + h * half, half)],
            agx_s.at[0, h, way], agx_r.at[0, h, way], fft=fright if way == 0 else fleft,
        )

    def agx1_here(h, way):
        owner = slab_of(nx - 1 if way == 0 else 1, c)
        return rc(
            u_hbm.at[rows(h * half, half)], ufull.at[rows(owner * slab + h * half, half)],
            agx_s.at[0, h, way], agx_r.at[0, h, way], fft=fright if way == 0 else fleft,
        )

    def agx2(way):
        owner = slab_of(nx - 1 if way == 0 else 1, c)
        piece = ufull.at[rows(owner * slab + way * half, half)]
        return rc(
            piece, piece, agx_s.at[1, 0, way], agx_r.at[1, 0, way],
            fft=fright if way == 0 else fleft,
        )

    def agx2_here(way):
        piece = ufull.at[rows(slab_of(2, c) * slab + way * half, half)]
        return rc(
            piece, piece, agx_s.at[1, 0, way], agx_r.at[1, 0, way],
            fft=fright if way == 0 else fleft,
        )

    def du(k, core):
        piece = ufull.at[rows(slab_of((0, nx - 1, 1, 2)[k], core) * slab, slab)]
        src = u_hbm if (k == 0) else piece
        return rc(src, piece, du_s.at[k], du_r.at[k], fft=mate)

    du(0, c).start()

    def agz(s, q, way):
        owner = (slot - (s - 1) + nb) % nb if way == 0 else (slot + (s - 1)) % nb
        piece = pfull.at[rows(place(owner) * slab + q * quarter, quarter)]
        return rc(
            piece, piece, agz_s.at[s, q, way], agz_r.at[s, q, way],
            band=right if way == 0 else left,
        )

    def agz_here(s, q, way):
        owner = (slot - s + nb) % nb if way == 0 else (slot + s) % nb
        piece = pfull.at[rows(place(owner) * slab + q * quarter, quarter)]
        return rc(
            piece, piece, agz_s.at[s, q, way], agz_r.at[s, q, way],
            band=right if way == 0 else left,
        )

    for q in range(quarters):
        @pl.when(jnp.logical_not(alone))
        def _():
            perm_here(q).wait_recv()

        @pl.when(alone)
        def _():
            perm_local(q).wait()

        for way in (0, 1):
            agz(1, q, way).start()

    for way in (0, 1):
        agx1(way, way).start()
    for way in (0, 1):
        agx1(1 - way, way).start()

    def forward(s, q):
        for way in (0, 1):
            agz_here(s - 1, q, way).wait_recv()
            agz(s, q, way).start()

    for q in range(quarters):
        forward(2, q)
    for way in (0, 1):
        agx1_here(way, way).wait_recv()
        agx2(way).start()
    for q in range(quarters):
        forward(3, q)
    for way in (0, 1):
        agx1_here(1 - way, way).wait_recv()
        du(1 + way, c).start()
    for way in (0, 1):
        agx2_here(way).wait_recv()
    du(3, c).start()
    u_local.wait()
    for k in range(4):
        du(k, 1 - c).wait_recv()

    first_lanes = lax.broadcasted_iota(jnp.int32, (1, width), 1) < width // 2
    batch = 4

    def forward_planes(owner, k):
        a, s = owner // nf, owner % nf
        p = pfull[rows(owner * slab + k * batch * n, batch * n), :]
        u = ufull[rows(s * slab + k * batch * n, batch * n), :]
        ps, us = swapped(p), swapped(u)
        real = jnp.where(first_lanes, p, ps)
        imag = jnp.where(first_lanes, ps, -p)
        rho = real * u + imag * us
        spec = along_last(rho, zf_ref[...])
        base = (a * n + s * planes + k * batch) * pitch
        for q in range(0, batch, 2):
            outs = along_left(
                [spec[q * n : (q + 1) * n], spec[(q + 1) * n : (q + 2) * n]], lf_ref[...]
            )
            for e in (0, 1):
                dbuf[rows(base + (q + e) * pitch, n), :] = outs[e]

    last = nb // 2

    per_slab = planes // batch

    def items_ready(t):
        ready = per_slab * (2 * (t // quarters + first - 2) + 1)
        return jnp.minimum(jnp.minimum(2 * (t + 1), ready), nb * per_slab)

    first = 4

    @pl.loop(0, quarters * (last + 2 - first) + 1)
    def _(t):
        s, q = first + t // quarters, t % quarters

        @pl.when(s < last)
        def _():
            forward(s, q)

        @pl.when(s == last)
        def _():
            for way in (0, 1):
                agz_here(s - 1, q, way).wait_recv()

                @pl.when(2 * q // quarters == way)
                def _():
                    agz(s, q, way).start()

        @pl.when(s == last + 1)
        def _():
            for way in (0, 1):
                @pl.when(2 * q // quarters == way)
                def _():
                    agz_here(last, q, way).wait_recv()

        @pl.loop(jnp.where(t == 0, 0, items_ready(t - 1)), items_ready(t))
        def _(w):
            order, k = w // per_slab, w % per_slab
            far = (order + 1) // 2
            owner = jnp.where(order % 2 == 1, slot + far, slot - far + nb) % nb
            forward_planes(place(owner), k)

    def a2a(src_of, dst, ssem, rsem, d):
        to = (b + d) % nb
        return rc(src_of(to), dst.at[rows(b * part, part)], ssem.at[d], rsem.at[d], band=to)

    def a2a_here(src_of, dst, ssem, rsem, d):
        to = (b + d) % nb
        source = (b - d + nb) % nb
        return rc(src_of(to), dst.at[rows(source * part, part)], ssem.at[d], rsem.at[d], band=to)

    au = (lambda t: u_hbm.at[rows(t * part, part)], usub, au_s, au_r)

    @pl.loop(1, nb)
    def _(i):
        a2a(*au, farthest_first(i, nb)).start()

    u_mine = pltpu.make_async_copy(
        u_hbm.at[rows(b * part, part)], usub.at[rows(b * part, part)], loc.at[1]
    )
    u_mine.start()

    freq = lax.broadcasted_iota(jnp.int32, (n, width), 0)
    freq = jnp.where(freq < n // 2, freq, freq - n).astype(F32)
    lane = lax.broadcasted_iota(jnp.int32, (n, width), 1) % n
    lane = jnp.where(lane < n // 2, lane, lane - n).astype(F32)
    shift = []
    for a in (0, 1):
        row = idx_ref[lead + nf * a]
        shift.append([tab_ref[e, row] for e in range(3)])
    for a in (0, 1):
        fx = freq + shift[a][0]
        fz = lane + shift[a][2]
        hops[rows(a * n, n), :] = fx * fx + fz * fz + SCREEN_SQUARE
    scale = FOUR_PI / n**3
    per = 8

    @pl.loop(0, n // per)
    def _(k):
        chains = [(a, k * per + e) for e in range(0, per, 2) for a in (0, 1)]
        taken, spectra = [], []
        for a, y in chains:
            take = [pl.ds(a * n * pitch + y + e, n, stride=pitch) for e in (0, 1)]
            taken.append(take)
            spectra.append(along_left([dbuf[t, :] for t in take], lf_ref[...]))
        screened = []
        for (a, y), pair in zip(chains, spectra):
            base = hops[pl.ds(a * n, n), :]
            both = []
            for e in (0, 1):
                fy = jnp.where(y + e < n // 2, y + e, y + e - n).astype(F32) + shift[a][1]
                both.append(pair[e] * (scale / (base + fy * fy)))
            screened.append(both)
        for take, both in zip(taken, screened):
            for t, field in zip(take, along_left(both, li_ref[...])):
                dbuf[t, :] = field

    def dv(k):
        src = vbuf.at[rows(slab_at(k, 1 - c) * slab, slab)]
        return rc(src, d2d.at[rows(k * slab, slab)], dv_s.at[k], dv_r.at[k], fft=mate)

    def slab_at(k, core):
        dx = jnp.where(k == 0, 2, jnp.where(k == 1, 1, jnp.where(k == 2, nx - 1, 0)))
        return slab_of(dx, core)

    def hop(k, src, way):
        return rc(
            src, hops.at[rows(2 * n + k * half, half)], rs_s.at[k], rs_r.at[k],
            fft=fright if way == 0 else fleft,
        )

    def piece(dx, h):
        return vbuf.at[rows(slab_of(dx, c) * slab + h * half, half)]

    def hop_of(k):
        way = k % 2
        toward = 1 if way == 0 else nx - 1
        if k < 2:
            return hop(k, piece(2, way), way)
        if k < 4:
            return hop(k, piece(toward, 1 - way), way)
        return hop(k, piece(toward, way), way)

    wide = planes

    def inverse_planes(s, k):
        total = None
        for a in (0, 1):
            base = (a * n + s * planes + k * wide) * pitch
            fields = []
            for q in range(0, wide, 2):
                fields += along_left(
                    [dbuf[rows(base + (q + e) * pitch, n), :] for e in (0, 1)], li_ref[...]
                )
            field = along_last(jnp.concatenate(fields, axis=0), zi_ref[...])
            p = pfull[rows((a * nf + s) * slab + k * wide * n, wide * n), :]
            ps = swapped(p)
            real = jnp.where(first_lanes, p, ps)
            imag = jnp.where(first_lanes, -ps, p)
            term = real * field + imag * swapped(field)
            total = term if total is None else total + term
        vbuf[rows(s * slab + k * wide * n, wide * n), :] = total

    @pl.loop(0, 2 * nx)
    def _(i):
        own = i >= nx
        k = i % nx
        s = slab_at(k, jnp.where(own, c, 1 - c))

        for q in range(planes // wide):
            inverse_planes(s, q)

        @pl.when(jnp.logical_not(own))
        def _():
            dv(k).start()

        @pl.when(own)
        def _():
            dv(k).wait_recv()
            vbuf[rows(s * slab, slab), :] += d2d[rows(k * slab, slab), :]

        @pl.when(i == nx)
        def _():
            hop_of(0).start()
            hop_of(1).start()

        @pl.when(i == nx + 1)
        def _():
            hop_of(2).start()

        @pl.when(i == nx + 2)
        def _():
            hop_of(3).start()

    def arrived(k):
        return hops[rows(2 * n + k * half, half), :]

    for way in (0, 1):
        hop_of(way).wait_recv()
        toward = slab_of(1 if way == 0 else nx - 1, c)
        vbuf[rows(toward * slab + way * half, half), :] += arrived(way)
        hop_of(4 + way).start()
    for k in (2, 3, 4, 5):
        hop_of(k).wait_recv()
    pot_ref[0:half, :] = vbuf[rows(f * slab, half), :] + arrived(3) + arrived(4)
    pot_ref[half:slab, :] = vbuf[rows(f * slab + half, half), :] + arrived(2) + arrived(5)

    av = (lambda t: pot_ref.at[rows(t * part, part)], vsub, av_s, av_r)

    @pl.loop(1, nb)
    def _(i):
        a2a(*av, farthest_first(i, nb)).start()

    vsub[rows(b * part, part), :] = pot_ref[rows(b * part, part), :]
    u_mine.wait()

    @pl.loop(1, nb)
    def _(d):
        a2a_here(*au, d).wait_recv()

    @pl.loop(1, nb)
    def _(d):
        a2a_here(*av, d).wait_recv()

    group = 4
    acc = jnp.zeros((2 * nb, 4 * nb), F32)
    for g in range(0, part, group):
        us = [usub[pl.ds(g + e, nb, stride=part), :] for e in range(group)]
        vs = [vsub[pl.ds(g + e, nb, stride=part), :] for e in range(group)]
        uh, ul = halves(jnp.concatenate(us, axis=1))
        vh, vl = halves(jnp.concatenate(vs, axis=1))
        th, tl = halves(jnp.concatenate([turned(v) for v in vs], axis=1))
        acc += lax.dot_general(
            jnp.concatenate([uh, ul], axis=0), jnp.concatenate([vh, th, vl, tl], axis=0),
            (((1,), (1,)), ((), ())), preferred_element_type=F32,
        )
    acc = acc[:nb] + acc[nb:]
    acc = (acc[:, : 2 * nb] + acc[:, 2 * nb :]) * (1.0 / n**3)
    folds = width // (2 * nb)
    tall = nb // folds
    mine[...] = jnp.concatenate([acc[k * tall : (k + 1) * tall] for k in range(folds)], axis=1)

    def mf(d, here=False):
        to = (f + d) % nf
        source = (f - d + nf) % nf
        at = source if here else f
        return rc(mine, mrow.at[at], mf_s.at[d], mf_r.at[d], fft=to)

    def mb(d, here=False):
        to = (b + d) % nb
        source = (b - d + nb) % nb
        at = source if here else b
        return rc(mcol, mall.at[at], mb_s.at[d], mb_r.at[d], band=to)

    for i in range(1, nf):
        mf(nf // 2 + (i // 2 if i % 2 == 0 else -(i // 2))).start()
    mrow[f] = mine[...]
    for d in range(1, nf):
        mf(d, True).wait_recv()
    total = mrow[0]
    for k in range(1, nf):
        total += mrow[k]
    mcol[...] = total

    @pl.loop(1, nb)
    def _(i):
        mb(farthest_first(i, nb)).start()

    mall[b] = mcol[...]

    @pl.loop(1, nb)
    def _(d):
        mb(d, True).wait_recv()

    total = mall[0]
    for k in range(1, nb):
        total += mall[k]
    total = jnp.concatenate(
        [total[:, 2 * nb * k : 2 * nb * (k + 1)] for k in range(folds)], axis=0
    )

    ri = lax.broadcasted_iota(jnp.int32, (nb, nb), 0)
    ci = lax.broadcasted_iota(jnp.int32, (nb, nb), 1)
    eye = (ri == ci).astype(F32)

    def flipped(m):
        return lax.dot_general(
            eye, m, (((1,), (1,)), ((), ())), precision=lax.Precision.HIGHEST,
            preferred_element_type=F32,
        )

    mre, mim = total[:, :nb], total[:, nb : 2 * nb]
    hre = jnp.where(ri >= ci, mre, flipped(mre))
    him = jnp.where(ri > ci, mim, jnp.where(ri < ci, -flipped(mim), 0.0))
    zero = jnp.zeros((nb, nb), F32)
    work = jnp.concatenate([hre, him, eye, zero], axis=1)
    other = jnp.concatenate([-him, hre, zero, eye], axis=1)
    row_at = lax.broadcasted_iota(jnp.int32, (nb, 1), 0)
    for k in range(nb):
        pivot = work[k : k + 1, k : k + 1]
        cre = jnp.where(row_at > k, work[:, k : k + 1], 0.0) / pivot
        cim = jnp.where(row_at > k, work[:, nb + k : nb + k + 1], 0.0) / pivot
        row, rot = work[k : k + 1, :], other[k : k + 1, :]
        work = work - (cre * row + cim * rot)
        other = other - (cre * rot - cim * row)
    pivots = jnp.sum(work[:, :nb] * eye, axis=1, keepdims=True)
    coef = work[:, 2 * nb : 4 * nb] / jnp.sqrt(pivots)
    ch, cl = halves(coef)
    coef = jnp.concatenate(
        [jnp.concatenate([ch, ch], axis=1), jnp.concatenate([cl, cl], axis=1)], axis=0
    )

    for g in range(0, part, group):
        vs = [vsub[pl.ds(g + e, nb, stride=part), :] for e in range(group)]
        cols = jnp.concatenate([left_column(v) for v in vs], axis=1)
        both = mm(coef, cols)
        out = both[:nb] + both[nb:]
        for e in range(group):
            psub[pl.ds(g + e, nb, stride=part), :] = out[:, e * width : (e + 1) * width]

    ap = (lambda t: psub.at[rows(t * part, part)], proj_ref, ap_s, ap_r)

    @pl.loop(1, nb)
    def _(i):
        a2a(*ap, farthest_first(i, nb)).start()

    proj_ref[rows(b * part, part), :] = psub[rows(b * part, part), :]

    @pl.when(jnp.logical_not(alone))
    def _():
        for q in range(quarters):
            perm(q).wait_send()

    for way in (0, 1):
        for h in (0, 1):
            agx1(h, way).wait_send()
        agx2(way).wait_send()
    for k in range(4):
        du(k, c).wait_send()

    @pl.loop(1, last)
    def _(s):
        for q in range(quarters):
            for way in (0, 1):
                agz(s, q, way).wait_send()

    for q in range(quarters):
        agz(last, q, 2 * q // quarters).wait_send()

    @pl.loop(0, nx)
    def _(k):
        dv(k).wait_send()

    for k in range(6):
        hop_of(k).wait_send()
    for d in range(1, nf):
        mf(d).wait_send()

    @pl.loop(1, nb)
    def _(d):
        a2a(*au, d).wait_send()
        a2a(*av, d).wait_send()
        mb(d).wait_send()
        a2a(*ap, d).wait_send()

    @pl.loop(1, nb)
    def _(d):
        a2a_here(*ap, d).wait_recv()


def body(mesh, orbitals, partners, shift_table, shift_index):
    nb, nf = mesh.shape["band"], mesh.shape["fft"]
    n = orbitals.shape[2]
    width = orbitals.shape[3]
    slab = orbitals.shape[0] * orbitals.shape[1] * n
    part = slab // nb
    assert nb == 2 * nf and nf == 8 and SPREAD**2 % nf == 1 and orbitals.shape[0] == 1

    def call(p, u, *rest):
        any_spec = pl.BlockSpec(memory_space=pl.ANY)
        vmem = pl.BlockSpec(memory_space=pltpu.VMEM)
        smem = pl.BlockSpec(memory_space=pltpu.SMEM)
        dma = pltpu.SemaphoreType.DMA
        out = jax.ShapeDtypeStruct((slab, width), F32)
        half = slab // 2
        tall = 2 * nb * nb // width
        return pl.pallas_call(
            lambda *refs: kernel(nb, nf, n, *refs),
            out_shape=(out, out),
            in_specs=[any_spec, any_spec, vmem, vmem, vmem, vmem, smem, smem],
            out_specs=(vmem, vmem),
            scratch_shapes=[
                pltpu.VMEM((nb * slab, width), F32),
                pltpu.VMEM((nf * slab, width), F32),
                pltpu.VMEM((2 * n * (n + PAD), width), F32),
                pltpu.VMEM((nf * slab, width), F32),
                pltpu.VMEM((nf // 2 * slab, width), F32),
                pltpu.VMEM((2 * n + 6 * half, width), F32),
                pltpu.VMEM((slab, width), F32),
                pltpu.VMEM((slab, width), F32),
                pltpu.VMEM((slab, width), F32),
                pltpu.VMEM((tall, width), F32),
                pltpu.VMEM((nf, tall, width), F32),
                pltpu.VMEM((tall, width), F32),
                pltpu.VMEM((nb, tall, width), F32),
                dma((4,)), dma((4,)), dma((6,)),
                dma((nb // 2 + 1, 4, 2)), dma((nb // 2 + 1, 4, 2)),
                dma((2, 2, 2)), dma((2, 2, 2)),
                dma((4,)), dma((4,)), dma((4,)), dma((4,)), dma((6,)), dma((6,)),
                dma((nb,)), dma((nb,)), dma((nb,)), dma((nb,)), dma((nb,)), dma((nb,)),
                dma((nf,)), dma((nf,)), dma((nb,)), dma((nb,)),
            ],
            compiler_params=pltpu.CompilerParams(collective_id=0, has_side_effects=True),
            name="exchange",
        )(p, u, *rest)

    tables = [
        jnp.asarray(t)
        for t in (last_table(n, -1.0), last_table(n, 1.0), left_table(n, -1.0), left_table(n, 1.0))
    ]
    pot, proj = call(
        partners.reshape(slab, width), orbitals.reshape(slab, width), *tables,
        shift_table.T, shift_index,
    )
    return pot.reshape(orbitals.shape), proj.reshape(orbitals.shape)


def solution(mesh):
    spec = P(("kgrp", "band"), "fft", None, None)
    return jax.shard_map(
        lambda *args: body(mesh, *args), mesh=mesh, in_specs=(spec, spec, P(), P("kgrp")),
        out_specs=(spec, spec), check_vma=False,
    )
```

```python
import math

import jax
import jax.numpy as jnp
import numpy as np
from jax import lax
from jax.experimental import pallas as pl
from jax.experimental.pallas import tpu as pltpu
from jax.sharding import PartitionSpec as P

SCREEN_SQUARE = 0.25
FOUR_PI = 4.0 * math.pi
MESH = pl.DeviceIdType.MESH
SPREAD = 5
PAD = 8
BF = jnp.bfloat16
F32 = jnp.float32


def split_table(table):
    high = np.asarray(table, np.float64).astype(jnp.bfloat16)
    low = (np.asarray(table, np.float64) - high.astype(np.float64)).astype(jnp.bfloat16)
    return high, low


def dft(extent):
    k = np.arange(extent)
    angle = 2.0 * np.pi * ((k[:, None] * k[None, :]) % extent) / extent
    return np.cos(angle), np.sin(angle)


def last_table(extent, sign):
    cosine, sine = dft(extent)
    sine = sign * sine
    table = np.block([[cosine, sine], [-sine, cosine]])
    high, low = split_table(table)
    both = np.concatenate([high, low], axis=1)
    return np.concatenate([both, both], axis=0)


def left_table(extent, sign):
    cosine, sine = dft(extent)
    table = np.concatenate([cosine, -sign * sine], axis=1)
    high, low = split_table(table)
    return np.concatenate(
        [np.concatenate([high, high], axis=1), np.concatenate([low, low], axis=1)], axis=0
    )


def halves(v):
    high = v.astype(BF)
    low = (v - high.astype(F32)).astype(BF)
    return high, low


def swapped(v):
    return pltpu.roll(v, v.shape[-1] // 2, 1)


def lane_sign(shape, first, second):
    lane = lax.broadcasted_iota(jnp.int32, shape, len(shape) - 1)
    return jnp.where(lane < shape[-1] // 2, first, second).astype(F32)


def turned(v):
    return swapped(v) * lane_sign((1, v.shape[-1]), 1.0, -1.0)


def mm(a, b):
    return jnp.dot(a, b, preferred_element_type=F32)


def along_last(v, table):
    high, low = halves(v)
    width = v.shape[-1]
    both = mm(jnp.concatenate([high, low], axis=1), table)
    return both[:, :width] + both[:, width:]


def left_column(v):
    high, low = halves(v)
    thigh, tlow = halves(turned(v))
    return jnp.concatenate([high, thigh, low, tlow], axis=0)


def along_left(blocks, table):
    rows = table.shape[0] // 2
    columns = jnp.concatenate([left_column(v) for v in blocks], axis=1)
    both = mm(table, columns)
    out = both[:rows] + both[rows:]
    width = blocks[0].shape[-1]
    return [out[:, k * width : (k + 1) * width] for k in range(len(blocks))]


def kernel(
    nb, nf, n, p_hbm, u_hbm, zf_ref, zi_ref, lf_ref, li_ref, tab_ref, idx_ref,
    pot_ref, proj_ref,
    pfull, ufull, dbuf, vbuf, d2d, hops, usub, vsub, psub, mine, mrow, mcol, mall,
    perm_r, loc, agz_r, agx_r, du_r, dv_r, rs_r, many,
):
    slab = p_hbm.shape[0]
    half = slab // 2
    quarters = 4
    quarter = slab // quarters
    planes = slab // n
    width = p_hbm.shape[1]
    nx = nf // 2
    part = slab // nb
    pitch = n + PAD
    b = lax.axis_index("band")
    f = lax.axis_index("fft")
    x, c = f // 2, f % 2
    mate = f + 1 - 2 * c
    right, left = (b + 1) % nb, (b + nb - 1) % nb
    fright, fleft = (f + 2) % nf, (f + nf - 2) % nf
    lead = x + nx * c
    slot = (b - lead + nf // 2 + nb) % nb
    to_band = (b - nf // 2 + (SPREAD * f) % nf + nb) % nb
    to_fft = 2 * (b % nx) + (b // nx) % 2
    to_slot = (b // nf) * nf + f
    from_fft = (SPREAD * slot) % nf
    from_band = lead + nf * (slot // nf)
    alone = jnp.logical_and(to_band == b, to_fft == f)

    def farthest_first(i, count):
        return count // 2 + jnp.where(i % 2 == 0, i // 2, -(i // 2))

    def rows(start, count):
        return pl.ds(pl.multiple_of(start, 8), count)

    def rc(src, dst, ssem, rsem, **dev):
        return pltpu.make_async_remote_copy(
            src_ref=src, dst_ref=dst, send_sem=ssem, recv_sem=rsem, device_id=dev,
            device_id_type=MESH,
        )

    perm_s, agz_s, agx_s, du_s, dv_s, rs_s = [many.at[k] for k in range(6)]
    au_s, av_s, ap_s, mf_s, mb_s = [many.at[k] for k in range(6, 11)]
    au_r, av_r, ap_r, mf_r, mb_r = [many.at[k] for k in range(11, 16)]

    def all_sent(ref, sem):
        rc(ref, ref, sem, sem, fft=mate).wait_send()

    def all_here(ref, sem):
        rc(ref, ref, sem, sem, fft=mate).wait_recv()

    barrier = pltpu.get_barrier_semaphore()

    def greet(**dev):
        pl.semaphore_signal(barrier, inc=1, device_id=dev, device_id_type=MESH)

    greet(band=right)
    greet(band=left)
    greet(fft=fright)
    greet(fft=fleft)
    greet(fft=mate)

    @pl.when(jnp.logical_not(alone))
    def _():
        greet(band=to_band, fft=to_fft)
        greet(band=from_band, fft=from_fft)

    u_local = pltpu.make_async_copy(u_hbm, ufull.at[rows(f * slab, slab)], loc.at[0])
    u_local.start()
    pl.semaphore_wait(barrier, jnp.where(alone, 5, 7))

    def place(at):
        return (at // nf) * nf + (SPREAD * at) % nf

    def perm(q):
        return rc(
            p_hbm.at[rows(q * quarter, quarter)],
            pfull.at[rows(to_slot * slab + q * quarter, quarter)],
            perm_s, perm_r.at[q], band=to_band, fft=to_fft,
        )

    def perm_here(q):
        return rc(
            p_hbm.at[rows(q * quarter, quarter)],
            pfull.at[rows(place(slot) * slab + q * quarter, quarter)],
            perm_s, perm_r.at[q], band=from_band, fft=from_fft,
        )

    def perm_local(q):
        return pltpu.make_async_copy(
            p_hbm.at[rows(q * quarter, quarter)],
            pfull.at[rows(place(slot) * slab + q * quarter, quarter)], loc.at[2 + q],
        )

    @pl.when(jnp.logical_not(alone))
    def _():
        for q in range(quarters):
            perm(q).start()

    @pl.when(alone)
    def _():
        for q in range(quarters):
            perm_local(q).start()

    def slab_of(dx, core):
        return 2 * ((x + dx) % nx) + core

    def agx1(h, way):
        return rc(
            u_hbm.at[rows(h * half, half)], ufull.at[rows(f * slab + h * half, half)],
            agx_s, agx_r.at[0, h, way], fft=fright if way == 0 else fleft,
        )

    def agx1_here(h, way):
        owner = slab_of(nx - 1 if way == 0 else 1, c)
        return rc(
            u_hbm.at[rows(h * half, half)], ufull.at[rows(owner * slab + h * half, half)],
            agx_s, agx_r.at[0, h, way], fft=fright if way == 0 else fleft,
        )

    def agx2(way):
        owner = slab_of(nx - 1 if way == 0 else 1, c)
        piece = ufull.at[rows(owner * slab + way * half, half)]
        return rc(
            piece, piece, agx_s, agx_r.at[1, 0, way],
            fft=fright if way == 0 else fleft,
        )

    def agx2_here(way):
        piece = ufull.at[rows(slab_of(2, c) * slab + way * half, half)]
        return rc(
            piece, piece, agx_s, agx_r.at[1, 0, way],
            fft=fright if way == 0 else fleft,
        )

    def du(k, core):
        piece = ufull.at[rows(slab_of((0, nx - 1, 1, 2)[k], core) * slab, slab)]
        src = u_hbm if (k == 0) else piece
        return rc(src, piece, du_s, du_r.at[k], fft=mate)

    du(0, c).start()

    def agz(s, q, way):
        owner = (slot - (s - 1) + nb) % nb if way == 0 else (slot + (s - 1)) % nb
        piece = pfull.at[rows(place(owner) * slab + q * quarter, quarter)]
        return rc(
            piece, piece, agz_s, agz_r.at[s, q, way],
            band=right if way == 0 else left,
        )

    def agz_here(s, q, way):
        owner = (slot - s + nb) % nb if way == 0 else (slot + s) % nb
        piece = pfull.at[rows(place(owner) * slab + q * quarter, quarter)]
        return rc(
            piece, piece, agz_s, agz_r.at[s, q, way],
            band=right if way == 0 else left,
        )

    for q in range(quarters):
        @pl.when(jnp.logical_not(alone))
        def _():
            perm_here(q).wait_recv()

        @pl.when(alone)
        def _():
            perm_local(q).wait()

        for way in (0, 1):
            agz(1, q, way).start()

    for way in (0, 1):
        agx1(way, way).start()
    for way in (0, 1):
        agx1(1 - way, way).start()

    def forward(s, q):
        for way in (0, 1):
            agz_here(s - 1, q, way).wait_recv()
            agz(s, q, way).start()

    for q in range(quarters):
        forward(2, q)
    for way in (0, 1):
        agx1_here(way, way).wait_recv()
        agx2(way).start()
    for q in range(quarters):
        forward(3, q)
    for way in (0, 1):
        agx1_here(1 - way, way).wait_recv()
        du(1 + way, c).start()
    for q in range(quarters):
        forward(4, q)
    for way in (0, 1):
        agx2_here(way).wait_recv()
    du(3, c).start()
    u_local.wait()
    for k in range(4):
        du(k, 1 - c).wait_recv()

    first_lanes = lax.broadcasted_iota(jnp.int32, (1, width), 1) < width // 2
    batch = 4

    def forward_planes(owner, k):
        a, s = owner // nf, owner % nf
        p = pfull[rows(owner * slab + k * batch * n, batch * n), :]
        u = ufull[rows(s * slab + k * batch * n, batch * n), :]
        ps, us = swapped(p), swapped(u)
        real = jnp.where(first_lanes, p, ps)
        imag = jnp.where(first_lanes, ps, -p)
        rho = real * u + imag * us
        spec = along_last(rho, zf_ref[...])
        base = (a * n + s * planes + k * batch) * pitch
        for q in range(0, batch, 2):
            outs = along_left(
                [spec[q * n : (q + 1) * n], spec[(q + 1) * n : (q + 2) * n]], lf_ref[...]
            )
            for e in (0, 1):
                dbuf[rows(base + (q + e) * pitch, n), :] = outs[e]

    last = nb // 2

    per_slab = planes // batch

    def items_ready(t):
        ready = per_slab * (2 * (t // quarters + first - 2) + 1)
        return jnp.minimum(jnp.minimum(2 * (t + 1), ready), nb * per_slab)

    first = 5

    @pl.loop(0, quarters * (last + 2 - first) + 1)
    def _(t):
        s, q = first + t // quarters, t % quarters

        @pl.when(s < last)
        def _():
            forward(s, q)

        @pl.when(s == last)
        def _():
            for way in (0, 1):
                agz_here(s - 1, q, way).wait_recv()

                @pl.when(2 * q // quarters == way)
                def _():
                    agz(s, q, way).start()

        @pl.when(s == last + 1)
        def _():
            for way in (0, 1):
                @pl.when(2 * q // quarters == way)
                def _():
                    agz_here(last, q, way).wait_recv()

        @pl.loop(jnp.where(t == 0, 0, items_ready(t - 1)), items_ready(t))
        def _(w):
            order, k = w // per_slab, w % per_slab
            far = (order + 1) // 2
            owner = jnp.where(order % 2 == 1, slot + far, slot - far + nb) % nb
            forward_planes(place(owner), k)

    bit = part // 2

    def in_slab(t, h):
        return rows(h * half + t * bit, bit)

    def in_parts(t, h):
        return rows(t * part + h * bit, bit)

    def spread(src, dst, ssem, rsem, h, d):
        to = (b + d) % nb
        return rc(src.at[in_slab(to, h)], dst.at[in_parts(b, h)], ssem, rsem, band=to)

    def gather(h, d):
        to = (b + d) % nb
        return rc(psub.at[in_parts(to, h)], proj_ref.at[in_slab(b, h)], ap_s, ap_r, band=to)

    au = (u_hbm, usub, au_s, au_r)
    av = (pot_ref, vsub, av_s, av_r)

    @pl.loop(1, nb)
    def _(i):
        for h in (0, 1):
            spread(*au, h, farthest_first(i, nb)).start()

    def u_mine(h):
        return pltpu.make_async_copy(
            u_hbm.at[in_slab(b, h)], usub.at[in_parts(b, h)], loc.at[1 if h == 0 else 6]
        )

    for h in (0, 1):
        u_mine(h).start()

    freq = lax.broadcasted_iota(jnp.int32, (n, width), 0)
    freq = jnp.where(freq < n // 2, freq, freq - n).astype(F32)
    lane = lax.broadcasted_iota(jnp.int32, (n, width), 1) % n
    lane = jnp.where(lane < n // 2, lane, lane - n).astype(F32)
    shift = []
    for a in (0, 1):
        row = idx_ref[lead + nf * a]
        shift.append([tab_ref[e, row] for e in range(3)])
    for a in (0, 1):
        fx = freq + shift[a][0]
        fz = lane + shift[a][2]
        hops[rows(a * n, n), :] = fx * fx + fz * fz + SCREEN_SQUARE
    scale = FOUR_PI / n**3
    per = 8

    @pl.loop(0, n // per)
    def _(k):
        chains = [(a, k * per + e) for e in range(0, per, 2) for a in (0, 1)]
        taken, spectra = [], []
        for a, y in chains:
            take = [pl.ds(a * n * pitch + y + e, n, stride=pitch) for e in (0, 1)]
            taken.append(take)
            spectra.append(along_left([dbuf[t, :] for t in take], lf_ref[...]))
        screened = []
        for (a, y), pair in zip(chains, spectra):
            base = hops[pl.ds(a * n, n), :]
            both = []
            for e in (0, 1):
                fy = jnp.where(y + e < n // 2, y + e, y + e - n).astype(F32) + shift[a][1]
                both.append(pair[e] * (scale / (base + fy * fy)))
            screened.append(both)
        for take, both in zip(taken, screened):
            for t, field in zip(take, along_left(both, li_ref[...])):
                dbuf[t, :] = field

    order = (2, 1, nx - 1, 0)

    def dv(h, k):
        src = vbuf.at[rows(slab_of(order[k], 1 - c) * slab + h * half, half)]
        return rc(
            src, d2d.at[rows(k * slab + h * half, half)], dv_s, dv_r.at[h, k], fft=mate
        )

    def landing(h, k):
        return rows(2 * n + (h * 6 + k) * quarter, quarter)

    def own_rows(dx, h, e):
        return rows(slab_of(dx, c) * slab + h * half + e * quarter, quarter)

    def hop(h, k):
        way = k % 2
        toward = 1 if way == 0 else nx - 1
        piece = own_rows(2 if k < 2 else toward, h, 1 - way if k in (2, 3) else way)
        return rc(
            vbuf.at[piece], hops.at[landing(h, k)], rs_s, rs_r.at[h, k],
            fft=fright if way == 0 else fleft,
        )

    def inverse_halves(h, pair, core):
        at = [slab_of(order[k], core) for k in pair]
        total = None
        for a in (0, 1):
            fields = []
            for s in at:
                base = (a * n + s * planes + h * (planes // 2)) * pitch
                for e in range(0, planes // 2, 2):
                    fields += along_left(
                        [dbuf[rows(base + (e + g) * pitch, n), :] for g in (0, 1)], li_ref[...]
                    )
            field = along_last(jnp.concatenate(fields, axis=0), zi_ref[...])
            p = jnp.concatenate(
                [pfull[rows((a * nf + s) * slab + h * half, half), :] for s in at], axis=0
            )
            ps = swapped(p)
            real = jnp.where(first_lanes, p, ps)
            imag = jnp.where(first_lanes, -ps, p)
            term = real * field + imag * swapped(field)
            total = term if total is None else total + term
        for k, s in enumerate(at):
            vbuf[rows(s * slab + h * half, half), :] = total[k * half : (k + 1) * half]

    def relay(h):
        for way in (0, 1):
            hop(h, way).wait_recv()
            toward = own_rows(1 if way == 0 else nx - 1, h, way)
            vbuf[toward, :] += hops[landing(h, way), :]
            hop(h, 4 + way).start()

    def with_mate(h, k):
        dv(h, k).wait_recv()
        own = rows(slab_of(order[k], c) * slab + h * half, half)
        vbuf[own, :] += d2d[rows(k * slab + h * half, half), :]

    @pl.loop(0, 2)
    def _(h):
        inverse_halves(h, (0, 1), 1 - c)
        dv(h, 0).start()
        dv(h, 1).start()
        inverse_halves(h, (0, 1), c)
        inverse_halves(h, (2, 3), 1 - c)
        dv(h, 2).start()
        dv(h, 3).start()

        @pl.when(h == 1)
        def _():
            relay(0)

        with_mate(h, 0)
        hop(h, 0).start()
        hop(h, 1).start()
        with_mate(h, 1)
        hop(h, 2).start()
        inverse_halves(h, (2, 3), c)
        with_mate(h, 2)
        hop(h, 3).start()
        with_mate(h, 3)

    for h in (0, 1):
        if h == 1:
            relay(1)
        for k in (2, 3, 4, 5):
            hop(h, k).wait_recv()
        pot_ref[rows(h * half, quarter), :] = (
            vbuf[own_rows(0, h, 0), :] + hops[landing(h, 3), :] + hops[landing(h, 4), :]
        )
        pot_ref[rows(h * half + quarter, quarter), :] = (
            vbuf[own_rows(0, h, 1), :] + hops[landing(h, 2), :] + hops[landing(h, 5), :]
        )

        @pl.loop(1, nb)
        def _(m):
            spread(*av, h, farthest_first(m, nb)).start()

    for h in (0, 1):
        vsub[in_parts(b, h), :] = pot_ref[in_slab(b, h), :]
        u_mine(h).wait()

    others = pl.ds(0, (nb - 1) * part)
    all_here(usub.at[others], au_r)
    all_here(vsub.at[others], av_r)

    group = 4
    acc = jnp.zeros((2 * nb, 4 * nb), F32)
    for g in range(0, part, group):
        us = [usub[pl.ds(g + e, nb, stride=part), :] for e in range(group)]
        vs = [vsub[pl.ds(g + e, nb, stride=part), :] for e in range(group)]
        uh, ul = halves(jnp.concatenate(us, axis=1))
        vh, vl = halves(jnp.concatenate(vs, axis=1))
        th, tl = halves(jnp.concatenate([turned(v) for v in vs], axis=1))
        acc += lax.dot_general(
            jnp.concatenate([uh, ul], axis=0), jnp.concatenate([vh, th, vl, tl], axis=0),
            (((1,), (1,)), ((), ())), preferred_element_type=F32,
        )
    acc = acc[:nb] + acc[nb:]
    acc = (acc[:, : 2 * nb] + acc[:, 2 * nb :]) * (1.0 / n**3)
    folds = width // (2 * nb)
    tall = nb // folds
    mine[...] = jnp.concatenate([acc[k * tall : (k + 1) * tall] for k in range(folds)], axis=1)

    def mf(d):
        to = (f + d) % nf
        return rc(mine, mrow.at[f], mf_s, mf_r, fft=to)

    def mb(d):
        to = (b + d) % nb
        return rc(mcol, mall.at[b], mb_s, mb_r, band=to)

    for i in range(1, nf):
        mf(nf // 2 + (i // 2 if i % 2 == 0 else -(i // 2))).start()
    mrow[f] = mine[...]
    all_here(mrow.at[pl.ds(0, nf - 1)], mf_r)
    total = mrow[0]
    for k in range(1, nf):
        total += mrow[k]
    mcol[...] = total

    @pl.loop(1, nb)
    def _(i):
        mb(farthest_first(i, nb)).start()

    mall[b] = mcol[...]

    all_here(mall.at[pl.ds(0, nb - 1)], mb_r)

    total = mall[0]
    for k in range(1, nb):
        total += mall[k]
    total = jnp.concatenate(
        [total[:, 2 * nb * k : 2 * nb * (k + 1)] for k in range(folds)], axis=0
    )

    ri = lax.broadcasted_iota(jnp.int32, (nb, nb), 0)
    ci = lax.broadcasted_iota(jnp.int32, (nb, nb), 1)
    eye = (ri == ci).astype(F32)

    def flipped(m):
        return lax.dot_general(
            eye, m, (((1,), (1,)), ((), ())), precision=lax.Precision.HIGHEST,
            preferred_element_type=F32,
        )

    mre, mim = total[:, :nb], total[:, nb : 2 * nb]
    hre = jnp.where(ri >= ci, mre, flipped(mre))
    him = jnp.where(ri > ci, mim, jnp.where(ri < ci, -flipped(mim), 0.0))
    zero = jnp.zeros((nb, nb), F32)
    work = jnp.concatenate([hre, him, eye, zero], axis=1)
    other = jnp.concatenate([-him, hre, zero, eye], axis=1)
    row_at = lax.broadcasted_iota(jnp.int32, (nb, 1), 0)
    for k in range(nb):
        pivot = work[k : k + 1, k : k + 1]
        cre = jnp.where(row_at > k, work[:, k : k + 1], 0.0) / pivot
        cim = jnp.where(row_at > k, work[:, nb + k : nb + k + 1], 0.0) / pivot
        row, rot = work[k : k + 1, :], other[k : k + 1, :]
        work = work - (cre * row + cim * rot)
        other = other - (cre * rot - cim * row)
    pivots = jnp.sum(work[:, :nb] * eye, axis=1, keepdims=True)
    coef = work[:, 2 * nb : 4 * nb] / jnp.sqrt(pivots)
    ch, cl = halves(coef)
    coef = jnp.concatenate(
        [jnp.concatenate([ch, ch], axis=1), jnp.concatenate([cl, cl], axis=1)], axis=0
    )

    for g in range(0, part, group):
        vs = [vsub[pl.ds(g + e, nb, stride=part), :] for e in range(group)]
        cols = jnp.concatenate([left_column(v) for v in vs], axis=1)
        both = mm(coef, cols)
        out = both[:nb] + both[nb:]
        for e in range(group):
            psub[pl.ds(g + e, nb, stride=part), :] = out[:, e * width : (e + 1) * width]

    @pl.loop(1, nb)
    def _(i):
        for h in (0, 1):
            gather(h, farthest_first(i, nb)).start()

    for h in (0, 1):
        proj_ref[in_slab(b, h), :] = psub[in_parts(b, h), :]

    @pl.when(jnp.logical_not(alone))
    def _():
        all_sent(pfull.at[pl.ds(0, slab)], perm_s)

    all_sent(pfull.at[pl.ds(0, (nb - 1) * slab)], agz_s)
    all_sent(ufull.at[pl.ds(0, (nx - 1) * slab)], agx_s)
    all_sent(ufull.at[pl.ds(0, nx * slab)], du_s)
    all_sent(vbuf.at[pl.ds(0, nx * slab)], dv_s)
    all_sent(vbuf.at[pl.ds(0, (nx - 1) * slab)], rs_s)
    all_sent(usub.at[others], au_s)
    all_sent(vsub.at[others], av_s)
    all_sent(mrow.at[pl.ds(0, nf - 1)], mf_s)
    all_sent(mall.at[pl.ds(0, nb - 1)], mb_s)
    all_sent(psub.at[others], ap_s)
    all_here(proj_ref.at[others], ap_r)


def body(mesh, orbitals, partners, shift_table, shift_index):
    nb, nf = mesh.shape["band"], mesh.shape["fft"]
    n = orbitals.shape[2]
    width = orbitals.shape[3]
    slab = orbitals.shape[0] * orbitals.shape[1] * n
    part = slab // nb
    assert nb == 2 * nf and nf == 8 and SPREAD**2 % nf == 1 and orbitals.shape[0] == 1

    def call(p, u, *rest):
        any_spec = pl.BlockSpec(memory_space=pl.ANY)
        vmem = pl.BlockSpec(memory_space=pltpu.VMEM)
        smem = pl.BlockSpec(memory_space=pltpu.SMEM)
        dma = pltpu.SemaphoreType.DMA
        out = pltpu.VMEM((slab, width), F32)
        half = slab // 2
        tall = 2 * nb * nb // width
        return pl.pallas_call(
            lambda *refs: kernel(nb, nf, n, *refs),
            out_shape=(out, out),
            in_specs=[any_spec, any_spec, vmem, vmem, vmem, vmem, smem, smem],
            out_specs=(vmem, vmem),
            scratch_shapes=[
                pltpu.VMEM((nb * slab, width), F32),
                pltpu.VMEM((nf * slab, width), F32),
                pltpu.VMEM((2 * n * (n + PAD), width), F32),
                pltpu.VMEM((nf * slab, width), F32),
                pltpu.VMEM((nf // 2 * slab, width), F32),
                pltpu.VMEM((2 * n + 6 * half, width), F32),
                pltpu.VMEM((slab, width), F32),
                pltpu.VMEM((slab, width), F32),
                pltpu.VMEM((slab, width), F32),
                pltpu.VMEM((tall, width), F32),
                pltpu.VMEM((nf, tall, width), F32),
                pltpu.VMEM((tall, width), F32),
                pltpu.VMEM((nb, tall, width), F32),
                dma((4,)), dma((7,)), dma((nb // 2 + 1, 4, 2)), dma((2, 2, 2)), dma((4,)),
                dma((2, 4)), dma((2, 6)), dma((16,)),
            ],
            compiler_params=pltpu.CompilerParams(collective_id=0, has_side_effects=True),
            name="exchange",
        )(p, u, *rest)

    tables = [
        jnp.asarray(t)
        for t in (last_table(n, -1.0), last_table(n, 1.0), left_table(n, -1.0), left_table(n, 1.0))
    ]
    pot, proj = call(
        partners.reshape(slab, width), orbitals.reshape(slab, width), *tables,
        shift_table.T, shift_index,
    )
    return pot.reshape(orbitals.shape), proj.reshape(orbitals.shape)


def solution(mesh):
    spec = P(("kgrp", "band"), "fft", None, None)
    return jax.shard_map(
        lambda *args: body(mesh, *args), mesh=mesh, in_specs=(spec, spec, P(), P("kgrp")),
        out_specs=(spec, spec), check_vma=False,
    )
```

```python
import math

import jax
import jax.numpy as jnp
import numpy as np
from jax import lax
from jax.experimental import pallas as pl
from jax.experimental.pallas import tpu as pltpu
from jax.sharding import PartitionSpec as P

SCREEN_SQUARE = 0.25
FOUR_PI = 4.0 * math.pi
MESH = pl.DeviceIdType.MESH
SPREAD = 5
PAD = 8
BF = jnp.bfloat16
F32 = jnp.float32


def split_table(table):
    high = np.asarray(table, np.float64).astype(jnp.bfloat16)
    low = (np.asarray(table, np.float64) - high.astype(np.float64)).astype(jnp.bfloat16)
    return high, low


def dft(extent):
    k = np.arange(extent)
    angle = 2.0 * np.pi * ((k[:, None] * k[None, :]) % extent) / extent
    return np.cos(angle), np.sin(angle)


def last_table(extent, sign):
    cosine, sine = dft(extent)
    sine = sign * sine
    table = np.block([[cosine, sine], [-sine, cosine]])
    high, low = split_table(table)
    both = np.concatenate([high, low], axis=1)
    return np.concatenate([both, both], axis=0)


def left_table(extent, sign):
    cosine, sine = dft(extent)
    table = np.concatenate([cosine, -sign * sine], axis=1)
    high, low = split_table(table)
    return np.concatenate(
        [np.concatenate([high, high], axis=1), np.concatenate([low, low], axis=1)], axis=0
    )


def halves(v):
    high = v.astype(BF)
    low = (v - high.astype(F32)).astype(BF)
    return high, low


def swapped(v):
    return pltpu.roll(v, v.shape[-1] // 2, 1)


def lane_sign(shape, first, second):
    lane = lax.broadcasted_iota(jnp.int32, shape, len(shape) - 1)
    return jnp.where(lane < shape[-1] // 2, first, second).astype(F32)


def turned(v):
    return swapped(v) * lane_sign((1, v.shape[-1]), 1.0, -1.0)


def mm(a, b):
    return jnp.dot(a, b, preferred_element_type=F32)


def along_last(v, table):
    high, low = halves(v)
    width = v.shape[-1]
    both = mm(jnp.concatenate([high, low], axis=1), table)
    return both[:, :width] + both[:, width:]


def left_column(v):
    high, low = halves(v)
    thigh, tlow = halves(turned(v))
    return jnp.concatenate([high, thigh, low, tlow], axis=0)


def along_left(blocks, table):
    rows = table.shape[0] // 2
    columns = jnp.concatenate([left_column(v) for v in blocks], axis=1)
    both = mm(table, columns)
    out = both[:rows] + both[rows:]
    width = blocks[0].shape[-1]
    return [out[:, k * width : (k + 1) * width] for k in range(len(blocks))]


def kernel(
    nb, nf, n, p_hbm, u_hbm, zf_hbm, zi_hbm, lf_hbm, li_hbm, tab_ref, idx_ref,
    pot_ref, proj_ref,
    zf_ref, zi_ref, lf_ref, li_ref, pfull, ufull, dbuf, vbuf, d2d, hops, usub, vsub, psub, mine, mrow, mcol, mall,
    perm_r, loc, agz_r, agx_r, du_r, dv_r, rs_r, many,
):
    slab = p_hbm.shape[0]
    half = slab // 2
    quarters = 4
    quarter = slab // quarters
    planes = slab // n
    width = p_hbm.shape[1]
    nx = nf // 2
    part = slab // nb
    pitch = n + PAD
    b = lax.axis_index("band")
    f = lax.axis_index("fft")
    x, c = f // 2, f % 2
    mate = f + 1 - 2 * c
    right, left = (b + 1) % nb, (b + nb - 1) % nb
    fright, fleft = (f + 2) % nf, (f + nf - 2) % nf
    lead = x + nx * c
    slot = (b - lead + nf // 2 + nb) % nb
    to_band = (b - nf // 2 + (SPREAD * f) % nf + nb) % nb
    to_fft = 2 * (b % nx) + (b // nx) % 2
    to_slot = (b // nf) * nf + f
    from_fft = (SPREAD * slot) % nf
    from_band = lead + nf * (slot // nf)
    alone = jnp.logical_and(to_band == b, to_fft == f)

    def farthest_first(i, count):
        return count // 2 + jnp.where(i % 2 == 0, i // 2, -(i // 2))

    def rows(start, count):
        return pl.ds(pl.multiple_of(start, 8), count)

    def rc(src, dst, ssem, rsem, **dev):
        return pltpu.make_async_remote_copy(
            src_ref=src, dst_ref=dst, send_sem=ssem, recv_sem=rsem, device_id=dev,
            device_id_type=MESH,
        )

    perm_s, agz_s, agx_s, du_s, dv_s, rs_s = [many.at[k] for k in range(6)]
    au_s, av_s, ap_s, mf_s, mb_s = [many.at[k] for k in range(6, 11)]
    au_r, av_r, ap_r, mf_r, mb_r = [many.at[k] for k in range(11, 16)]

    def all_sent(ref, sem):
        rc(ref, ref, sem, sem, fft=mate).wait_send()

    def all_here(ref, sem):
        rc(ref, ref, sem, sem, fft=mate).wait_recv()

    barrier = pltpu.get_barrier_semaphore()

    def greet(**dev):
        pl.semaphore_signal(barrier, inc=1, device_id=dev, device_id_type=MESH)

    greet(band=right)
    greet(band=left)
    greet(fft=fright)
    greet(fft=fleft)
    greet(fft=mate)

    @pl.when(jnp.logical_not(alone))
    def _():
        greet(band=to_band, fft=to_fft)
        greet(band=from_band, fft=from_fft)

    tables = [
        pltpu.make_async_copy(src, dst, loc.at[7 + k])
        for k, (src, dst) in enumerate(
            ((zf_hbm, zf_ref), (zi_hbm, zi_ref), (lf_hbm, lf_ref), (li_hbm, li_ref))
        )
    ]
    for table in tables:
        table.start()
    u_local = pltpu.make_async_copy(u_hbm, ufull.at[rows(f * slab, slab)], loc.at[0])
    u_local.start()
    pl.semaphore_wait(barrier, jnp.where(alone, 5, 7))

    def place(at):
        return (at // nf) * nf + (SPREAD * at) % nf

    def perm(q):
        return rc(
            p_hbm.at[rows(q * quarter, quarter)],
            pfull.at[rows(to_slot * slab + q * quarter, quarter)],
            perm_s, perm_r.at[q], band=to_band, fft=to_fft,
        )

    def perm_here(q):
        return rc(
            p_hbm.at[rows(q * quarter, quarter)],
            pfull.at[rows(place(slot) * slab + q * quarter, quarter)],
            perm_s, perm_r.at[q], band=from_band, fft=from_fft,
        )

    def perm_local(q):
        return pltpu.make_async_copy(
            p_hbm.at[rows(q * quarter, quarter)],
            pfull.at[rows(place(slot) * slab + q * quarter, quarter)], loc.at[2 + q],
        )

    @pl.when(jnp.logical_not(alone))
    def _():
        for q in range(quarters):
            perm(q).start()

    @pl.when(alone)
    def _():
        for q in range(quarters):
            perm_local(q).start()

    def slab_of(dx, core):
        return 2 * ((x + dx) % nx) + core

    def agx1(h, way):
        return rc(
            u_hbm.at[rows(h * half, half)], ufull.at[rows(f * slab + h * half, half)],
            agx_s, agx_r.at[0, h, way], fft=fright if way == 0 else fleft,
        )

    def agx1_here(h, way):
        owner = slab_of(nx - 1 if way == 0 else 1, c)
        return rc(
            u_hbm.at[rows(h * half, half)], ufull.at[rows(owner * slab + h * half, half)],
            agx_s, agx_r.at[0, h, way], fft=fright if way == 0 else fleft,
        )

    def agx2(way):
        owner = slab_of(nx - 1 if way == 0 else 1, c)
        piece = ufull.at[rows(owner * slab + way * half, half)]
        return rc(
            piece, piece, agx_s, agx_r.at[1, 0, way],
            fft=fright if way == 0 else fleft,
        )

    def agx2_here(way):
        piece = ufull.at[rows(slab_of(2, c) * slab + way * half, half)]
        return rc(
            piece, piece, agx_s, agx_r.at[1, 0, way],
            fft=fright if way == 0 else fleft,
        )

    def du(k, core):
        piece = ufull.at[rows(slab_of((0, nx - 1, 1, 2)[k], core) * slab, slab)]
        src = u_hbm if (k == 0) else piece
        return rc(src, piece, du_s, du_r.at[k], fft=mate)

    du(0, c).start()

    def agz(s, q, way):
        owner = (slot - (s - 1) + nb) % nb if way == 0 else (slot + (s - 1)) % nb
        piece = pfull.at[rows(place(owner) * slab + q * quarter, quarter)]
        return rc(
            piece, piece, agz_s, agz_r.at[s, q, way],
            band=right if way == 0 else left,
        )

    def agz_here(s, q, way):
        owner = (slot - s + nb) % nb if way == 0 else (slot + s) % nb
        piece = pfull.at[rows(place(owner) * slab + q * quarter, quarter)]
        return rc(
            piece, piece, agz_s, agz_r.at[s, q, way],
            band=right if way == 0 else left,
        )

    for q in range(quarters):
        @pl.when(jnp.logical_not(alone))
        def _():
            perm_here(q).wait_recv()

        @pl.when(alone)
        def _():
            perm_local(q).wait()

        for way in (0, 1):
            agz(1, q, way).start()

    for way in (0, 1):
        agx1(way, way).start()
    for way in (0, 1):
        agx1(1 - way, way).start()

    def forward(s, q):
        for way in (0, 1):
            agz_here(s - 1, q, way).wait_recv()
            agz(s, q, way).start()

    for q in range(quarters):
        forward(2, q)
    for way in (0, 1):
        agx1_here(way, way).wait_recv()
        agx2(way).start()
    for q in range(quarters):
        forward(3, q)
    for way in (0, 1):
        agx1_here(1 - way, way).wait_recv()
        du(1 + way, c).start()
    for q in range(quarters):
        forward(4, q)
    for way in (0, 1):
        agx2_here(way).wait_recv()
    du(3, c).start()
    u_local.wait()
    for table in tables:
        table.wait()
    for k in range(4):
        du(k, 1 - c).wait_recv()

    first_lanes = lax.broadcasted_iota(jnp.int32, (1, width), 1) < width // 2
    batch = 4

    def forward_planes(owner, k):
        a, s = owner // nf, owner % nf
        p = pfull[rows(owner * slab + k * batch * n, batch * n), :]
        u = ufull[rows(s * slab + k * batch * n, batch * n), :]
        ps, us = swapped(p), swapped(u)
        real = jnp.where(first_lanes, p, ps)
        imag = jnp.where(first_lanes, ps, -p)
        rho = real * u + imag * us
        spec = along_last(rho, zf_ref[...])
        base = (a * n + s * planes + k * batch) * pitch
        for q in range(0, batch, 2):
            outs = along_left(
                [spec[q * n : (q + 1) * n], spec[(q + 1) * n : (q + 2) * n]], lf_ref[...]
            )
            for e in (0, 1):
                dbuf[rows(base + (q + e) * pitch, n), :] = outs[e]

    last = nb // 2

    per_slab = planes // batch

    def items_ready(t):
        ready = per_slab * (2 * (t // quarters + first - 2) + 1)
        return jnp.minimum(jnp.minimum(2 * (t + 1), ready), nb * per_slab)

    first = 5

    def items(start, stop):
        @pl.loop(start, stop)
        def _(w):
            order, k = w // per_slab, w % per_slab
            far = (order + 1) // 2
            owner = jnp.where(order % 2 == 1, slot + far, slot - far + nb) % nb
            forward_planes(place(owner), k)

    @pl.loop(0, quarters * (last + 1 - first))
    def _(t):
        s, q = first + t // quarters, t % quarters

        @pl.when(s < last)
        def _():
            forward(s, q)

        @pl.when(s == last)
        def _():
            for way in (0, 1):
                agz_here(s - 1, q, way).wait_recv()

                @pl.when(2 * q // quarters == way)
                def _():
                    agz(s, q, way).start()

        items(jnp.where(t == 0, 0, items_ready(t - 1)), items_ready(t))

    bit = part // 2

    def in_slab(t, h):
        return rows(h * half + t * bit, bit)

    def in_parts(t, h):
        return rows(t * part + h * bit, bit)

    def spread(src, dst, ssem, rsem, h, d):
        to = (b + d) % nb
        return rc(src.at[in_slab(to, h)], dst.at[in_parts(b, h)], ssem, rsem, band=to)

    def gather(h, d):
        to = (b + d) % nb
        return rc(psub.at[in_parts(to, h)], proj_ref.at[in_slab(b, h)], ap_s, ap_r, band=to)

    au = (u_hbm, usub, au_s, au_r)
    av = (pot_ref, vsub, av_s, av_r)

    def u_mine(h):
        return pltpu.make_async_copy(
            u_hbm.at[in_slab(b, h)], usub.at[in_parts(b, h)], loc.at[1 if h == 0 else 6]
        )

    freq = lax.broadcasted_iota(jnp.int32, (n, width), 0)
    freq = jnp.where(freq < n // 2, freq, freq - n).astype(F32)
    lane = lax.broadcasted_iota(jnp.int32, (n, width), 1) % n
    lane = jnp.where(lane < n // 2, lane, lane - n).astype(F32)
    scale = FOUR_PI / n**3
    per = 16
    done = items_ready(quarters * (last + 1 - first) - 1)
    before = (nb - 1) * per_slab

    @pl.loop(0, 2)
    def _(m):
        @pl.when(m == 1)
        def _():
            for q in range(quarters):
                agz_here(last, q, 2 * q // quarters).wait_recv()

            @pl.loop(1, nb)
            def _(i):
                for h in (0, 1):
                    spread(*au, h, farthest_first(i, nb)).start()

            for h in (0, 1):
                u_mine(h).start()

        items(jnp.where(m == 0, done, before), jnp.where(m == 0, before, nb * per_slab))
        a = (slot // nf + m) % 2
        row = idx_ref[lead + nf * a]
        qx, qy, qz = [tab_ref[e, row] for e in range(3)]
        fx, fz = freq + qx, lane + qz
        hops[pl.ds(0, n), :] = fx * fx + fz * fz + SCREEN_SQUARE

        @pl.loop(0, n // per)
        def _(k):
            taken, spectra = [], []
            for y in range(0, per, 2):
                take = [pl.ds(a * n * pitch + k * per + y + e, n, stride=pitch) for e in (0, 1)]
                taken.append(take)
                spectra.append(along_left([dbuf[t, :] for t in take], lf_ref[...]))
            base = hops[pl.ds(0, n), :]
            screened = []
            for y, pair in zip(range(0, per, 2), spectra):
                both = []
                for e in (0, 1):
                    at = k * per + y + e
                    fy = jnp.where(at < n // 2, at, at - n).astype(F32) + qy
                    both.append(pair[e] * (scale / (base + fy * fy)))
                screened.append(both)
            for take, both in zip(taken, screened):
                for t, field in zip(take, along_left(both, li_ref[...])):
                    dbuf[t, :] = field

    order = (2, 1, nx - 1, 0)

    def dv(h, k):
        src = vbuf.at[rows(slab_of(order[k], 1 - c) * slab + h * half, half)]
        return rc(
            src, d2d.at[rows(k * slab + h * half, half)], dv_s, dv_r.at[h, k], fft=mate
        )

    def landing(h, k):
        return rows(2 * n + (h * 6 + k) * quarter, quarter)

    def own_rows(dx, h, e):
        return rows(slab_of(dx, c) * slab + h * half + e * quarter, quarter)

    def hop(h, k):
        way = k % 2
        toward = 1 if way == 0 else nx - 1
        piece = own_rows(2 if k < 2 else toward, h, 1 - way if k in (2, 3) else way)
        return rc(
            vbuf.at[piece], hops.at[landing(h, k)], rs_s, rs_r.at[h, k],
            fft=fright if way == 0 else fleft,
        )

    def inverse_halves(h, pair, core):
        at = [slab_of(order[k], core) for k in pair]
        total = None
        for a in (0, 1):
            fields = []
            for s in at:
                base = (a * n + s * planes + h * (planes // 2)) * pitch
                for e in range(0, planes // 2, 2):
                    fields += along_left(
                        [dbuf[rows(base + (e + g) * pitch, n), :] for g in (0, 1)], li_ref[...]
                    )
            field = along_last(jnp.concatenate(fields, axis=0), zi_ref[...])
            p = jnp.concatenate(
                [pfull[rows((a * nf + s) * slab + h * half, half), :] for s in at], axis=0
            )
            ps = swapped(p)
            real = jnp.where(first_lanes, p, ps)
            imag = jnp.where(first_lanes, -ps, p)
            term = real * field + imag * swapped(field)
            total = term if total is None else total + term
        for k, s in enumerate(at):
            vbuf[rows(s * slab + h * half, half), :] = total[k * half : (k + 1) * half]

    def relay(h):
        for way in (0, 1):
            hop(h, way).wait_recv()
            toward = own_rows(1 if way == 0 else nx - 1, h, way)
            vbuf[toward, :] += hops[landing(h, way), :]
            hop(h, 4 + way).start()

    def with_mate(h, k):
        dv(h, k).wait_recv()
        own = rows(slab_of(order[k], c) * slab + h * half, half)
        vbuf[own, :] += d2d[rows(k * slab + h * half, half), :]

    @pl.loop(0, 2)
    def _(h):
        inverse_halves(h, (0, 1), 1 - c)
        dv(h, 0).start()
        dv(h, 1).start()
        inverse_halves(h, (0, 1), c)
        inverse_halves(h, (2, 3), 1 - c)
        dv(h, 2).start()
        dv(h, 3).start()

        @pl.when(h == 1)
        def _():
            relay(0)

        with_mate(h, 0)
        hop(h, 0).start()
        hop(h, 1).start()
        with_mate(h, 1)
        hop(h, 2).start()
        inverse_halves(h, (2, 3), c)
        with_mate(h, 2)
        hop(h, 3).start()
        with_mate(h, 3)

    for h in (0, 1):
        if h == 1:
            relay(1)
        for k in (2, 3, 4, 5):
            hop(h, k).wait_recv()
        pot_ref[rows(h * half, quarter), :] = (
            vbuf[own_rows(0, h, 0), :] + hops[landing(h, 3), :] + hops[landing(h, 4), :]
        )
        pot_ref[rows(h * half + quarter, quarter), :] = (
            vbuf[own_rows(0, h, 1), :] + hops[landing(h, 2), :] + hops[landing(h, 5), :]
        )

        @pl.loop(1, nb)
        def _(m):
            spread(*av, h, farthest_first(m, nb)).start()

    for h in (0, 1):
        vsub[in_parts(b, h), :] = pot_ref[in_slab(b, h), :]
        u_mine(h).wait()

    others = pl.ds(0, (nb - 1) * part)
    all_here(usub.at[others], au_r)
    all_here(vsub.at[others], av_r)

    group = 4
    acc = jnp.zeros((2 * nb, 4 * nb), F32)
    for g in range(0, part, group):
        us = [usub[pl.ds(g + e, nb, stride=part), :] for e in range(group)]
        vs = [vsub[pl.ds(g + e, nb, stride=part), :] for e in range(group)]
        uh, ul = halves(jnp.concatenate(us, axis=1))
        vh, vl = halves(jnp.concatenate(vs, axis=1))
        th, tl = halves(jnp.concatenate([turned(v) for v in vs], axis=1))
        acc += lax.dot_general(
            jnp.concatenate([uh, ul], axis=0), jnp.concatenate([vh, th, vl, tl], axis=0),
            (((1,), (1,)), ((), ())), preferred_element_type=F32,
        )
    acc = acc[:nb] + acc[nb:]
    acc = (acc[:, : 2 * nb] + acc[:, 2 * nb :]) * (1.0 / n**3)
    folds = width // (2 * nb)
    tall = nb // folds
    mine[...] = jnp.concatenate([acc[k * tall : (k + 1) * tall] for k in range(folds)], axis=1)

    def mf(d):
        to = (f + d) % nf
        return rc(mine, mrow.at[f], mf_s, mf_r, fft=to)

    def mb(d):
        to = (b + d) % nb
        return rc(mcol, mall.at[b], mb_s, mb_r, band=to)

    for i in range(1, nf):
        mf(nf // 2 + (i // 2 if i % 2 == 0 else -(i // 2))).start()
    mrow[f] = mine[...]
    all_here(mrow.at[pl.ds(0, nf - 1)], mf_r)
    total = mrow[0]
    for k in range(1, nf):
        total += mrow[k]
    mcol[...] = total

    @pl.loop(1, nb)
    def _(i):
        mb(farthest_first(i, nb)).start()

    mall[b] = mcol[...]

    all_here(mall.at[pl.ds(0, nb - 1)], mb_r)

    total = mall[0]
    for k in range(1, nb):
        total += mall[k]
    total = jnp.concatenate(
        [total[:, 2 * nb * k : 2 * nb * (k + 1)] for k in range(folds)], axis=0
    )

    ri = lax.broadcasted_iota(jnp.int32, (nb, nb), 0)
    ci = lax.broadcasted_iota(jnp.int32, (nb, nb), 1)
    eye = (ri == ci).astype(F32)

    def flipped(m):
        return lax.dot_general(
            eye, m, (((1,), (1,)), ((), ())), precision=lax.Precision.HIGHEST,
            preferred_element_type=F32,
        )

    mre, mim = total[:, :nb], total[:, nb : 2 * nb]
    hre = jnp.where(ri >= ci, mre, flipped(mre))
    him = jnp.where(ri > ci, mim, jnp.where(ri < ci, -flipped(mim), 0.0))
    zero = jnp.zeros((nb, nb), F32)
    work = jnp.concatenate([hre, him, eye, zero], axis=1)
    other = jnp.concatenate([-him, hre, zero, eye], axis=1)
    below = lax.broadcasted_iota(jnp.int32, work.shape, 0)
    for k in range(nb):
        inverse = 1.0 / jnp.broadcast_to(work[k : k + 1, k : k + 1], (1, 4 * nb))
        row, rot = work[k : k + 1, :] * inverse, other[k : k + 1, :] * inverse
        cre = jnp.where(below > k, jnp.broadcast_to(work[:, k : k + 1], work.shape), 0.0)
        cim = jnp.where(
            below > k, jnp.broadcast_to(work[:, nb + k : nb + k + 1], work.shape), 0.0
        )
        work = work - (cre * row + cim * rot)
        other = other - (cre * rot - cim * row)
    pivots = jnp.sum(work[:, :nb] * eye, axis=1, keepdims=True)
    coef = work[:, 2 * nb : 4 * nb] / jnp.sqrt(pivots)
    ch, cl = halves(coef)
    coef = jnp.concatenate(
        [jnp.concatenate([ch, ch], axis=1), jnp.concatenate([cl, cl], axis=1)], axis=0
    )

    for g in range(0, part, group):
        vs = [vsub[pl.ds(g + e, nb, stride=part), :] for e in range(group)]
        cols = jnp.concatenate([left_column(v) for v in vs], axis=1)
        both = mm(coef, cols)
        out = both[:nb] + both[nb:]
        for e in range(group):
            psub[pl.ds(g + e, nb, stride=part), :] = out[:, e * width : (e + 1) * width]

    @pl.loop(1, nb)
    def _(i):
        for h in (0, 1):
            gather(h, farthest_first(i, nb)).start()

    for h in (0, 1):
        proj_ref[in_slab(b, h), :] = psub[in_parts(b, h), :]

    @pl.when(jnp.logical_not(alone))
    def _():
        all_sent(pfull.at[pl.ds(0, slab)], perm_s)

    all_sent(pfull.at[pl.ds(0, (nb - 1) * slab)], agz_s)
    all_sent(ufull.at[pl.ds(0, (nx - 1) * slab)], agx_s)
    all_sent(ufull.at[pl.ds(0, nx * slab)], du_s)
    all_sent(vbuf.at[pl.ds(0, nx * slab)], dv_s)
    all_sent(vbuf.at[pl.ds(0, (nx - 1) * slab)], rs_s)
    all_sent(usub.at[others], au_s)
    all_sent(vsub.at[others], av_s)
    all_sent(mrow.at[pl.ds(0, nf - 1)], mf_s)
    all_sent(mall.at[pl.ds(0, nb - 1)], mb_s)
    all_sent(psub.at[others], ap_s)
    all_here(proj_ref.at[others], ap_r)


def body(mesh, orbitals, partners, shift_table, shift_index):
    nb, nf = mesh.shape["band"], mesh.shape["fft"]
    n = orbitals.shape[2]
    width = orbitals.shape[3]
    slab = orbitals.shape[0] * orbitals.shape[1] * n
    part = slab // nb
    assert nb == 2 * nf and nf == 8 and SPREAD**2 % nf == 1 and orbitals.shape[0] == 1

    def call(p, u, *rest):
        any_spec = pl.BlockSpec(memory_space=pl.ANY)
        vmem = pl.BlockSpec(memory_space=pltpu.VMEM)
        smem = pl.BlockSpec(memory_space=pltpu.SMEM)
        dma = pltpu.SemaphoreType.DMA
        out = pltpu.VMEM((slab, width), F32)
        half = slab // 2
        tall = 2 * nb * nb // width
        return pl.pallas_call(
            lambda *refs: kernel(nb, nf, n, *refs),
            out_shape=(out, out),
            in_specs=[any_spec] * 6 + [smem, smem],
            out_specs=(vmem, vmem),
            scratch_shapes=[pltpu.VMEM(t.shape, BF) for t in rest[:4]] + [
                pltpu.VMEM((nb * slab, width), F32),
                pltpu.VMEM((nf * slab, width), F32),
                pltpu.VMEM((2 * n * (n + PAD), width), F32),
                pltpu.VMEM((nf * slab, width), F32),
                pltpu.VMEM((nf // 2 * slab, width), F32),
                pltpu.VMEM((2 * n + 6 * half, width), F32),
                pltpu.VMEM((slab, width), F32),
                pltpu.VMEM((slab, width), F32),
                pltpu.VMEM((slab, width), F32),
                pltpu.VMEM((tall, width), F32),
                pltpu.VMEM((nf, tall, width), F32),
                pltpu.VMEM((tall, width), F32),
                pltpu.VMEM((nb, tall, width), F32),
                dma((4,)), dma((11,)), dma((nb // 2 + 1, 4, 2)), dma((2, 2, 2)), dma((4,)),
                dma((2, 4)), dma((2, 6)), dma((16,)),
            ],
            compiler_params=pltpu.CompilerParams(collective_id=0, has_side_effects=True),
            name="exchange",
        )(p, u, *rest)

    tables = [
        jnp.asarray(t)
        for t in (last_table(n, -1.0), last_table(n, 1.0), left_table(n, -1.0), left_table(n, 1.0))
    ]
    pot, proj = call(
        partners.reshape(slab, width), orbitals.reshape(slab, width), *tables,
        shift_table.T, shift_index,
    )
    return pot.reshape(orbitals.shape), proj.reshape(orbitals.shape)


def solution(mesh):
    spec = P(("kgrp", "band"), "fft", None, None)
    return jax.shard_map(
        lambda *args: body(mesh, *args), mesh=mesh, in_specs=(spec, spec, P(), P("kgrp")),
        out_specs=(spec, spec), check_vma=False,
    )
```

```python
import math

import jax
import jax.numpy as jnp
import numpy as np
from jax import lax
from jax.experimental import pallas as pl
from jax.experimental.pallas import tpu as pltpu
from jax.sharding import PartitionSpec as P

SCREEN_SQUARE = 0.25
FOUR_PI = 4.0 * math.pi
MESH = pl.DeviceIdType.MESH
SPREAD = 5
PAD = 8
BF = jnp.bfloat16
F32 = jnp.float32


def split_table(table):
    high = np.asarray(table, np.float64).astype(jnp.bfloat16)
    low = (np.asarray(table, np.float64) - high.astype(np.float64)).astype(jnp.bfloat16)
    return high, low


def dft(extent):
    k = np.arange(extent)
    angle = 2.0 * np.pi * ((k[:, None] * k[None, :]) % extent) / extent
    return np.cos(angle), np.sin(angle)


def last_table(extent, sign):
    cosine, sine = dft(extent)
    sine = sign * sine
    table = np.block([[cosine, sine], [-sine, cosine]])
    high, low = split_table(table)
    both = np.concatenate([high, low], axis=1)
    return np.concatenate([both, both], axis=0)


def left_table(extent, sign):
    cosine, sine = dft(extent)
    table = np.concatenate([cosine, -sign * sine], axis=1)
    high, low = split_table(table)
    return np.concatenate(
        [np.concatenate([high, high], axis=1), np.concatenate([low, low], axis=1)], axis=0
    )


def halves(v):
    high = v.astype(BF)
    low = (v - high.astype(F32)).astype(BF)
    return high, low


def swapped(v):
    return pltpu.roll(v, v.shape[-1] // 2, 1)


def lane_sign(shape, first, second):
    lane = lax.broadcasted_iota(jnp.int32, shape, len(shape) - 1)
    return jnp.where(lane < shape[-1] // 2, first, second).astype(F32)


def turned(v):
    return swapped(v) * lane_sign((1, v.shape[-1]), 1.0, -1.0)


def mm(a, b):
    return jnp.dot(a, b, preferred_element_type=F32)


def along_last(v, table):
    high, low = halves(v)
    width = v.shape[-1]
    both = mm(jnp.concatenate([high, low], axis=1), table)
    return both[:, :width] + both[:, width:]


def left_column(v):
    high, low = halves(v)
    thigh, tlow = halves(turned(v))
    return jnp.concatenate([high, thigh, low, tlow], axis=0)


def along_left(blocks, table):
    rows = table.shape[0] // 2
    columns = jnp.concatenate([left_column(v) for v in blocks], axis=1)
    both = mm(table, columns)
    out = both[:rows] + both[rows:]
    width = blocks[0].shape[-1]
    return [out[:, k * width : (k + 1) * width] for k in range(len(blocks))]


def kernel(
    nb, nf, n, p_hbm, u_hbm, zf_hbm, zi_hbm, lf_hbm, li_hbm, tab_ref, idx_ref,
    pot_ref, proj_ref,
    zf_ref, zi_ref, lf_ref, li_ref, p_own, pfull, ufull, dbuf, vbuf, d2d, hops, usub, vsub, psub, mine, mrow, mcol, mall,
    perm_r, loc, agz_r, agx_r, du_r, dv_r, rs_r, many,
):
    slab = p_hbm.shape[0]
    half = slab // 2
    quarters = 4
    quarter = slab // quarters
    planes = slab // n
    width = p_hbm.shape[1]
    nx = nf // 2
    part = slab // nb
    pitch = n + PAD
    b = lax.axis_index("band")
    f = lax.axis_index("fft")
    x, c = f // 2, f % 2
    mate = f + 1 - 2 * c
    right, left = (b + 1) % nb, (b + nb - 1) % nb
    fright, fleft = (f + 2) % nf, (f + nf - 2) % nf
    lead = x + nx * c
    slot = (b - lead + nf // 2 + nb) % nb
    to_band = (b - nf // 2 + (SPREAD * f) % nf + nb) % nb
    to_fft = 2 * (b % nx) + (b // nx) % 2
    to_slot = (b // nf) * nf + f
    from_fft = (SPREAD * slot) % nf
    from_band = lead + nf * (slot // nf)
    alone = jnp.logical_and(to_band == b, to_fft == f)

    def farthest_first(i, count):
        return count // 2 + jnp.where(i % 2 == 0, i // 2, -(i // 2))

    def rows(start, count):
        return pl.ds(pl.multiple_of(start, 8), count)

    def rc(src, dst, ssem, rsem, **dev):
        return pltpu.make_async_remote_copy(
            src_ref=src, dst_ref=dst, send_sem=ssem, recv_sem=rsem, device_id=dev,
            device_id_type=MESH,
        )

    perm_s, agz_s, agx_s, du_s, dv_s, rs_s = [many.at[k] for k in range(6)]
    au_s, av_s, ap_s, mf_s, mb_s = [many.at[k] for k in range(6, 11)]
    au_r, av_r, ap_r, mf_r, mb_r = [many.at[k] for k in range(11, 16)]

    def all_sent(ref, sem):
        rc(ref, ref, sem, sem, fft=mate).wait_send()

    def all_here(ref, sem):
        rc(ref, ref, sem, sem, fft=mate).wait_recv()

    barrier = pltpu.get_barrier_semaphore()

    def greet(**dev):
        pl.semaphore_signal(barrier, inc=1, device_id=dev, device_id_type=MESH)

    greet(band=right)
    greet(band=left)
    greet(fft=fright)
    greet(fft=fleft)
    greet(fft=mate)

    @pl.when(jnp.logical_not(alone))
    def _():
        greet(band=to_band, fft=to_fft)
        greet(band=from_band, fft=from_fft)

    tables = [
        pltpu.make_async_copy(src, dst, loc.at[7 + k])
        for k, (src, dst) in enumerate(
            ((zf_hbm, zf_ref), (zi_hbm, zi_ref), (lf_hbm, lf_ref), (li_hbm, li_ref))
        )
    ]
    p_local = pltpu.make_async_copy(p_hbm, p_own, loc.at[11])
    p_local.start()
    for table in tables:
        table.start()
    u_local = pltpu.make_async_copy(u_hbm, ufull.at[rows(f * slab, slab)], loc.at[0])
    u_local.start()
    p_local.wait()
    pl.semaphore_wait(barrier, jnp.where(alone, 5, 7))

    def place(at):
        return (at // nf) * nf + (SPREAD * at) % nf

    def perm(q):
        return rc(
            p_own.at[rows(q * quarter, quarter)],
            pfull.at[rows(to_slot * slab + q * quarter, quarter)],
            perm_s, perm_r.at[q], band=to_band, fft=to_fft,
        )

    def perm_here(q):
        return rc(
            p_own.at[rows(q * quarter, quarter)],
            pfull.at[rows(place(slot) * slab + q * quarter, quarter)],
            perm_s, perm_r.at[q], band=from_band, fft=from_fft,
        )

    def perm_local(q):
        return pltpu.make_async_copy(
            p_hbm.at[rows(q * quarter, quarter)],
            pfull.at[rows(place(slot) * slab + q * quarter, quarter)], loc.at[2 + q],
        )

    @pl.when(jnp.logical_not(alone))
    def _():
        for q in range(quarters):
            perm(q).start()

    @pl.when(alone)
    def _():
        for q in range(quarters):
            perm_local(q).start()

    def slab_of(dx, core):
        return 2 * ((x + dx) % nx) + core

    def agx1(h, way):
        return rc(
            u_hbm.at[rows(h * half, half)], ufull.at[rows(f * slab + h * half, half)],
            agx_s, agx_r.at[0, h, way], fft=fright if way == 0 else fleft,
        )

    def agx1_here(h, way):
        owner = slab_of(nx - 1 if way == 0 else 1, c)
        return rc(
            u_hbm.at[rows(h * half, half)], ufull.at[rows(owner * slab + h * half, half)],
            agx_s, agx_r.at[0, h, way], fft=fright if way == 0 else fleft,
        )

    def agx2(way):
        owner = slab_of(nx - 1 if way == 0 else 1, c)
        piece = ufull.at[rows(owner * slab + way * half, half)]
        return rc(
            piece, piece, agx_s, agx_r.at[1, 0, way],
            fft=fright if way == 0 else fleft,
        )

    def agx2_here(way):
        piece = ufull.at[rows(slab_of(2, c) * slab + way * half, half)]
        return rc(
            piece, piece, agx_s, agx_r.at[1, 0, way],
            fft=fright if way == 0 else fleft,
        )

    def du(k, core):
        piece = ufull.at[rows(slab_of((0, nx - 1, 1, 2)[k], core) * slab, slab)]
        src = u_hbm if (k == 0) else piece
        return rc(src, piece, du_s, du_r.at[k], fft=mate)

    du(0, c).start()

    def agz(s, q, way):
        owner = (slot - (s - 1) + nb) % nb if way == 0 else (slot + (s - 1)) % nb
        piece = pfull.at[rows(place(owner) * slab + q * quarter, quarter)]
        return rc(
            piece, piece, agz_s, agz_r.at[s, q, way],
            band=right if way == 0 else left,
        )

    def agz_here(s, q, way):
        owner = (slot - s + nb) % nb if way == 0 else (slot + s) % nb
        piece = pfull.at[rows(place(owner) * slab + q * quarter, quarter)]
        return rc(
            piece, piece, agz_s, agz_r.at[s, q, way],
            band=right if way == 0 else left,
        )

    for q in range(quarters):
        @pl.when(jnp.logical_not(alone))
        def _():
            perm_here(q).wait_recv()

        @pl.when(alone)
        def _():
            perm_local(q).wait()

        for way in (0, 1):
            agz(1, q, way).start()

    for way in (0, 1):
        agx1(way, way).start()
    for way in (0, 1):
        agx1(1 - way, way).start()

    def forward(s, q):
        for way in (0, 1):
            agz_here(s - 1, q, way).wait_recv()
            agz(s, q, way).start()

    for q in range(quarters):
        forward(2, q)
    for way in (0, 1):
        agx1_here(way, way).wait_recv()
        agx2(way).start()
    for q in range(quarters):
        forward(3, q)
    for way in (0, 1):
        agx1_here(1 - way, way).wait_recv()
        du(1 + way, c).start()
    for q in range(quarters):
        forward(4, q)
    for way in (0, 1):
        agx2_here(way).wait_recv()
    du(3, c).start()
    u_local.wait()
    for table in tables:
        table.wait()
    for k in range(4):
        du(k, 1 - c).wait_recv()

    first_lanes = lax.broadcasted_iota(jnp.int32, (1, width), 1) < width // 2
    batch = 4

    def forward_planes(owner, k):
        a, s = owner // nf, owner % nf
        p = pfull[rows(owner * slab + k * batch * n, batch * n), :]
        u = ufull[rows(s * slab + k * batch * n, batch * n), :]
        ps, us = swapped(p), swapped(u)
        real = jnp.where(first_lanes, p, ps)
        imag = jnp.where(first_lanes, ps, -p)
        rho = real * u + imag * us
        spec = along_last(rho, zf_ref[...])
        base = (a * n + s * planes + k * batch) * pitch
        for q in range(0, batch, 2):
            outs = along_left(
                [spec[q * n : (q + 1) * n], spec[(q + 1) * n : (q + 2) * n]], lf_ref[...]
            )
            for e in (0, 1):
                dbuf[rows(base + (q + e) * pitch, n), :] = outs[e]

    last = nb // 2

    per_slab = planes // batch
    assert per_slab == 2 and quarters == 4

    def items_ready(t):
        q = t % quarters
        ready = 2 * (2 * (t // quarters + first - 2) + 1) + 2 * ((q + 1) // 2)
        return jnp.minimum(2 * (t + 1), ready)

    first = 5

    def items(start, stop):
        @pl.loop(start, stop)
        def _(w):
            far = (w + 2) // 4
            ends = jnp.logical_or(w < 2, w >= nb * per_slab - 2)
            k = jnp.where(ends, w % 2, (w - 2) // 2 % 2)
            owner = jnp.where(ends | (w % 2 == 0), slot + far, slot - far + nb) % nb
            forward_planes(place(owner), k)

    @pl.loop(0, quarters * (last + 1 - first))
    def _(t):
        s, q = first + t // quarters, t % quarters

        @pl.when(s < last)
        def _():
            forward(s, q)

        @pl.when(s == last)
        def _():
            for way in (0, 1):
                agz_here(s - 1, q, way).wait_recv()

                @pl.when(2 * q // quarters == way)
                def _():
                    agz(s, q, way).start()

        items(jnp.where(t == 0, 0, items_ready(t - 1)), items_ready(t))

    bit = part // 2

    def in_slab(t, h):
        return rows(h * half + t * bit, bit)

    def in_parts(t, h):
        return rows(t * part + h * bit, bit)

    def spread(src, dst, ssem, rsem, h, d):
        to = (b + d) % nb
        return rc(src.at[in_slab(to, h)], dst.at[in_parts(b, h)], ssem, rsem, band=to)

    def gather(h, d):
        to = (b + d) % nb
        return rc(psub.at[in_parts(to, h)], proj_ref.at[in_slab(b, h)], ap_s, ap_r, band=to)

    au = (u_hbm, usub, au_s, au_r)
    av = (pot_ref, vsub, av_s, av_r)

    def u_mine(h):
        return pltpu.make_async_copy(
            u_hbm.at[in_slab(b, h)], usub.at[in_parts(b, h)], loc.at[1 if h == 0 else 6]
        )

    freq = lax.broadcasted_iota(jnp.int32, (n, width), 0)
    freq = jnp.where(freq < n // 2, freq, freq - n).astype(F32)
    lane = lax.broadcasted_iota(jnp.int32, (n, width), 1) % n
    lane = jnp.where(lane < n // 2, lane, lane - n).astype(F32)
    scale = FOUR_PI / n**3
    per = 16
    done = items_ready(quarters * (last + 1 - first) - 1)
    before = (nb - 1) * per_slab

    def orbital_parts(start, stop):
        @pl.loop(start, stop)
        def _(i):
            for h in (0, 1):
                spread(*au, h, farthest_first(i, nb)).start()

    @pl.loop(0, 2)
    def _(m):
        @pl.when(m == 1)
        def _():
            for q in range(quarters):
                agz_here(last, q, 2 * q // quarters).wait_recv()
            orbital_parts(last, nb)

        items(jnp.where(m == 0, done, before), jnp.where(m == 0, before, nb * per_slab))
        a = (slot // nf + m) % 2
        row = idx_ref[lead + nf * a]
        qx, qy, qz = [tab_ref[e, row] for e in range(3)]
        fx, fz = freq + qx, lane + qz
        hops[pl.ds(0, n), :] = fx * fx + fz * fz + SCREEN_SQUARE

        @pl.loop(0, n // per)
        def _(k):
            taken, spectra = [], []
            for y in range(0, per, 2):
                take = [pl.ds(a * n * pitch + k * per + y + e, n, stride=pitch) for e in (0, 1)]
                taken.append(take)
                spectra.append(along_left([dbuf[t, :] for t in take], lf_ref[...]))
            base = hops[pl.ds(0, n), :]
            screened = []
            for y, pair in zip(range(0, per, 2), spectra):
                both = []
                for e in (0, 1):
                    at = k * per + y + e
                    fy = jnp.where(at < n // 2, at, at - n).astype(F32) + qy
                    both.append(pair[e] * (scale / (base + fy * fy)))
                screened.append(both)
            for take, both in zip(taken, screened):
                for t, field in zip(take, along_left(both, li_ref[...])):
                    dbuf[t, :] = field

    order = (2, 1, nx - 1, 0)

    orbital_parts(1, last)
    for h in (0, 1):
        u_mine(h).start()

    def dv(h, k):
        src = vbuf.at[rows(slab_of(order[k], 1 - c) * slab + h * half, half)]
        return rc(
            src, d2d.at[rows(k * slab + h * half, half)], dv_s, dv_r.at[h, k], fft=mate
        )

    def landing(h, k):
        return rows(2 * n + (h * 6 + k) * quarter, quarter)

    def own_rows(dx, h, e):
        return rows(slab_of(dx, c) * slab + h * half + e * quarter, quarter)

    def hop(h, k):
        way = k % 2
        toward = 1 if way == 0 else nx - 1
        piece = own_rows(2 if k < 2 else toward, h, 1 - way if k in (2, 3) else way)
        return rc(
            vbuf.at[piece], hops.at[landing(h, k)], rs_s, rs_r.at[h, k],
            fft=fright if way == 0 else fleft,
        )

    def inverse_halves(h, pair, core):
        at = [slab_of(order[k], core) for k in pair]
        total = None
        for a in (0, 1):
            fields = []
            for s in at:
                base = (a * n + s * planes + h * (planes // 2)) * pitch
                for e in range(0, planes // 2, 2):
                    fields += along_left(
                        [dbuf[rows(base + (e + g) * pitch, n), :] for g in (0, 1)], li_ref[...]
                    )
            field = along_last(jnp.concatenate(fields, axis=0), zi_ref[...])
            p = jnp.concatenate(
                [pfull[rows((a * nf + s) * slab + h * half, half), :] for s in at], axis=0
            )
            ps = swapped(p)
            real = jnp.where(first_lanes, p, ps)
            imag = jnp.where(first_lanes, -ps, p)
            term = real * field + imag * swapped(field)
            total = term if total is None else total + term
        for k, s in enumerate(at):
            vbuf[rows(s * slab + h * half, half), :] = total[k * half : (k + 1) * half]

    def relay(h):
        for way in (0, 1):
            hop(h, way).wait_recv()
            toward = own_rows(1 if way == 0 else nx - 1, h, way)
            vbuf[toward, :] += hops[landing(h, way), :]
            hop(h, 4 + way).start()

    def with_mate(h, k):
        dv(h, k).wait_recv()
        own = rows(slab_of(order[k], c) * slab + h * half, half)
        vbuf[own, :] += d2d[rows(k * slab + h * half, half), :]

    @pl.loop(0, 2)
    def _(h):
        inverse_halves(h, (0, 1), 1 - c)
        dv(h, 0).start()
        dv(h, 1).start()
        inverse_halves(h, (0, 1), c)
        inverse_halves(h, (2, 3), 1 - c)
        dv(h, 2).start()
        dv(h, 3).start()

        @pl.when(h == 1)
        def _():
            relay(0)

        with_mate(h, 0)
        hop(h, 0).start()
        hop(h, 1).start()
        with_mate(h, 1)
        hop(h, 2).start()
        inverse_halves(h, (2, 3), c)
        with_mate(h, 2)
        hop(h, 3).start()
        with_mate(h, 3)

    for h in (0, 1):
        if h == 1:
            relay(1)
        for k in (2, 3, 4, 5):
            hop(h, k).wait_recv()
        pot_ref[rows(h * half, quarter), :] = (
            vbuf[own_rows(0, h, 0), :] + hops[landing(h, 3), :] + hops[landing(h, 4), :]
        )
        pot_ref[rows(h * half + quarter, quarter), :] = (
            vbuf[own_rows(0, h, 1), :] + hops[landing(h, 2), :] + hops[landing(h, 5), :]
        )

        @pl.loop(1, nb)
        def _(m):
            spread(*av, h, farthest_first(m, nb)).start()

    for h in (0, 1):
        vsub[in_parts(b, h), :] = pot_ref[in_slab(b, h), :]
        u_mine(h).wait()

    others = pl.ds(0, (nb - 1) * part)
    all_here(usub.at[others], au_r)
    all_here(vsub.at[others], av_r)

    group = 4
    acc = jnp.zeros((2 * nb, 4 * nb), F32)
    for g in range(0, part, group):
        us = [usub[pl.ds(g + e, nb, stride=part), :] for e in range(group)]
        vs = [vsub[pl.ds(g + e, nb, stride=part), :] for e in range(group)]
        uh, ul = halves(jnp.concatenate(us, axis=1))
        vh, vl = halves(jnp.concatenate(vs, axis=1))
        th, tl = halves(jnp.concatenate([turned(v) for v in vs], axis=1))
        acc += lax.dot_general(
            jnp.concatenate([uh, ul], axis=0), jnp.concatenate([vh, th, vl, tl], axis=0),
            (((1,), (1,)), ((), ())), preferred_element_type=F32,
        )
    acc = acc[:nb] + acc[nb:]
    acc = (acc[:, : 2 * nb] + acc[:, 2 * nb :]) * (1.0 / n**3)
    folds = width // (2 * nb)
    tall = nb // folds
    mine[...] = jnp.concatenate([acc[k * tall : (k + 1) * tall] for k in range(folds)], axis=1)

    def mf(d):
        to = (f + d) % nf
        return rc(mine, mrow.at[f], mf_s, mf_r, fft=to)

    def mb(d):
        to = (b + d) % nb
        return rc(mcol, mall.at[b], mb_s, mb_r, band=to)

    for i in range(1, nf):
        mf(nf // 2 + (i // 2 if i % 2 == 0 else -(i // 2))).start()
    mrow[f] = mine[...]
    all_here(mrow.at[pl.ds(0, nf - 1)], mf_r)
    total = mrow[0]
    for k in range(1, nf):
        total += mrow[k]
    mcol[...] = total

    @pl.loop(1, nb)
    def _(i):
        mb(farthest_first(i, nb)).start()

    mall[b] = mcol[...]

    all_here(mall.at[pl.ds(0, nb - 1)], mb_r)

    total = mall[0]
    for k in range(1, nb):
        total += mall[k]
    total = jnp.concatenate(
        [total[:, 2 * nb * k : 2 * nb * (k + 1)] for k in range(folds)], axis=0
    )

    ri = lax.broadcasted_iota(jnp.int32, (nb, nb), 0)
    ci = lax.broadcasted_iota(jnp.int32, (nb, nb), 1)
    eye = (ri == ci).astype(F32)

    def flipped(m):
        return lax.dot_general(
            eye, m, (((1,), (1,)), ((), ())), precision=lax.Precision.HIGHEST,
            preferred_element_type=F32,
        )

    mre, mim = total[:, :nb], total[:, nb : 2 * nb]
    hre = jnp.where(ri >= ci, mre, flipped(mre))
    him = jnp.where(ri > ci, mim, jnp.where(ri < ci, -flipped(mim), 0.0))
    zero = jnp.zeros((nb, nb), F32)
    work = jnp.concatenate([hre, him, eye, zero], axis=1)
    other = jnp.concatenate([-him, hre, zero, eye], axis=1)
    below = lax.broadcasted_iota(jnp.int32, work.shape, 0)
    for k in range(nb):
        inverse = 1.0 / jnp.broadcast_to(work[k : k + 1, k : k + 1], (1, 4 * nb))
        row, rot = work[k : k + 1, :] * inverse, other[k : k + 1, :] * inverse
        cre = jnp.where(below > k, jnp.broadcast_to(work[:, k : k + 1], work.shape), 0.0)
        cim = jnp.where(
            below > k, jnp.broadcast_to(work[:, nb + k : nb + k + 1], work.shape), 0.0
        )
        work = work - (cre * row + cim * rot)
        other = other - (cre * rot - cim * row)
    pivots = jnp.sum(work[:, :nb] * eye, axis=1, keepdims=True)
    coef = work[:, 2 * nb : 4 * nb] / jnp.sqrt(pivots)
    ch, cl = halves(coef)
    coef = jnp.concatenate(
        [jnp.concatenate([ch, ch], axis=1), jnp.concatenate([cl, cl], axis=1)], axis=0
    )

    for g in range(0, part, group):
        vs = [vsub[pl.ds(g + e, nb, stride=part), :] for e in range(group)]
        cols = jnp.concatenate([left_column(v) for v in vs], axis=1)
        both = mm(coef, cols)
        out = both[:nb] + both[nb:]
        for e in range(group):
            psub[pl.ds(g + e, nb, stride=part), :] = out[:, e * width : (e + 1) * width]

    @pl.loop(1, nb)
    def _(i):
        for h in (0, 1):
            gather(h, farthest_first(i, nb)).start()

    for h in (0, 1):
        proj_ref[in_slab(b, h), :] = psub[in_parts(b, h), :]

    @pl.when(jnp.logical_not(alone))
    def _():
        all_sent(pfull.at[pl.ds(0, slab)], perm_s)

    all_sent(pfull.at[pl.ds(0, (nb - 1) * slab)], agz_s)
    all_sent(ufull.at[pl.ds(0, (nx - 1) * slab)], agx_s)
    all_sent(ufull.at[pl.ds(0, nx * slab)], du_s)
    all_sent(vbuf.at[pl.ds(0, nx * slab)], dv_s)
    all_sent(vbuf.at[pl.ds(0, (nx - 1) * slab)], rs_s)
    all_sent(usub.at[others], au_s)
    all_sent(vsub.at[others], av_s)
    all_sent(mrow.at[pl.ds(0, nf - 1)], mf_s)
    all_sent(mall.at[pl.ds(0, nb - 1)], mb_s)
    all_sent(psub.at[others], ap_s)
    all_here(proj_ref.at[others], ap_r)


def body(mesh, orbitals, partners, shift_table, shift_index):
    nb, nf = mesh.shape["band"], mesh.shape["fft"]
    n = orbitals.shape[2]
    width = orbitals.shape[3]
    slab = orbitals.shape[0] * orbitals.shape[1] * n
    part = slab // nb
    assert nb == 2 * nf and nf == 8 and SPREAD**2 % nf == 1 and orbitals.shape[0] == 1

    def call(p, u, *rest):
        any_spec = pl.BlockSpec(memory_space=pl.ANY)
        vmem = pl.BlockSpec(memory_space=pltpu.VMEM)
        smem = pl.BlockSpec(memory_space=pltpu.SMEM)
        dma = pltpu.SemaphoreType.DMA
        out = pltpu.VMEM((slab, width), F32)
        half = slab // 2
        tall = 2 * nb * nb // width
        return pl.pallas_call(
            lambda *refs: kernel(nb, nf, n, *refs),
            out_shape=(out, out),
            in_specs=[any_spec] * 6 + [smem, smem],
            out_specs=(vmem, vmem),
            scratch_shapes=[pltpu.VMEM(t.shape, BF) for t in rest[:4]] + [
                pltpu.VMEM((slab, width), F32),
                pltpu.VMEM((nb * slab, width), F32),
                pltpu.VMEM((nf * slab, width), F32),
                pltpu.VMEM((2 * n * (n + PAD), width), F32),
                pltpu.VMEM((nf * slab, width), F32),
                pltpu.VMEM((nf // 2 * slab, width), F32),
                pltpu.VMEM((2 * n + 6 * half, width), F32),
                pltpu.VMEM((slab, width), F32),
                pltpu.VMEM((slab, width), F32),
                pltpu.VMEM((slab, width), F32),
                pltpu.VMEM((tall, width), F32),
                pltpu.VMEM((nf, tall, width), F32),
                pltpu.VMEM((tall, width), F32),
                pltpu.VMEM((nb, tall, width), F32),
                dma((4,)), dma((12,)), dma((nb // 2 + 1, 4, 2)), dma((2, 2, 2)), dma((4,)),
                dma((2, 4)), dma((2, 6)), dma((16,)),
            ],
            compiler_params=pltpu.CompilerParams(collective_id=0, has_side_effects=True),
            name="exchange",
        )(p, u, *rest)

    tables = [
        jnp.asarray(t)
        for t in (last_table(n, -1.0), last_table(n, 1.0), left_table(n, -1.0), left_table(n, 1.0))
    ]
    pot, proj = call(
        partners.reshape(slab, width), orbitals.reshape(slab, width), *tables,
        shift_table.T, shift_index,
    )
    return pot.reshape(orbitals.shape), proj.reshape(orbitals.shape)


def solution(mesh):
    spec = P(("kgrp", "band"), "fft", None, None)
    return jax.shard_map(
        lambda *args: body(mesh, *args), mesh=mesh, in_specs=(spec, spec, P(), P("kgrp")),
        out_specs=(spec, spec), check_vma=False,
    )
```

```python
import math

import jax
import jax.numpy as jnp
import numpy as np
from jax import lax
from jax.experimental import pallas as pl
from jax.experimental.pallas import tpu as pltpu
from jax.sharding import PartitionSpec as P

SCREEN_SQUARE = 0.25
FOUR_PI = 4.0 * math.pi
MESH = pl.DeviceIdType.MESH
SPREAD = 5
PAD = 8
BF = jnp.bfloat16
F32 = jnp.float32


def split_table(table):
    high = np.asarray(table, np.float64).astype(jnp.bfloat16)
    low = (np.asarray(table, np.float64) - high.astype(np.float64)).astype(jnp.bfloat16)
    return high, low


def dft(extent):
    k = np.arange(extent)
    angle = 2.0 * np.pi * ((k[:, None] * k[None, :]) % extent) / extent
    return np.cos(angle), np.sin(angle)


def last_table(extent, sign):
    cosine, sine = dft(extent)
    sine = sign * sine
    table = np.block([[cosine, sine], [-sine, cosine]])
    high, low = split_table(table)
    both = np.concatenate([high, low], axis=1)
    return np.concatenate([both, both], axis=0)


def left_table(extent, sign):
    cosine, sine = dft(extent)
    table = np.concatenate([cosine, -sign * sine], axis=1)
    high, low = split_table(table)
    return np.concatenate(
        [np.concatenate([high, high], axis=1), np.concatenate([low, low], axis=1)], axis=0
    )


def halves(v):
    high = v.astype(BF)
    low = (v - high.astype(F32)).astype(BF)
    return high, low


def swapped(v):
    return pltpu.roll(v, v.shape[-1] // 2, 1)


def lane_sign(shape, first, second):
    lane = lax.broadcasted_iota(jnp.int32, shape, len(shape) - 1)
    return jnp.where(lane < shape[-1] // 2, first, second).astype(F32)


def turned(v):
    return swapped(v) * lane_sign((1, v.shape[-1]), 1.0, -1.0)


def mm(a, b):
    return jnp.dot(a, b, preferred_element_type=F32)


def along_last(v, table):
    high, low = halves(v)
    width = v.shape[-1]
    both = mm(jnp.concatenate([high, low], axis=1), table)
    return both[:, :width] + both[:, width:]


def left_column(v):
    high, low = halves(v)
    thigh, tlow = halves(turned(v))
    return jnp.concatenate([high, thigh, low, tlow], axis=0)


def along_left(blocks, table):
    rows = table.shape[0] // 2
    columns = jnp.concatenate([left_column(v) for v in blocks], axis=1)
    both = mm(table, columns)
    out = both[:rows] + both[rows:]
    width = blocks[0].shape[-1]
    return [out[:, k * width : (k + 1) * width] for k in range(len(blocks))]


def kernel(
    nb, nf, n, p_hbm, u_hbm, zf_hbm, zi_hbm, lf_hbm, li_hbm, tab_ref, idx_ref,
    pot_ref, proj_ref,
    zf_ref, zi_ref, lf_ref, li_ref, p_own, pfull, ufull, dbuf, vbuf, d2d, hops, usub, vsub, psub, mine, mrow, mcol, mall,
    perm_r, loc, agz_r, agx_r, du_r, dv_r, rs_r, many,
):
    slab = p_hbm.shape[0]
    half = slab // 2
    quarters = 4
    quarter = slab // quarters
    planes = slab // n
    width = p_hbm.shape[1]
    nx = nf // 2
    part = slab // nb
    pitch = n + PAD
    b = lax.axis_index("band")
    f = lax.axis_index("fft")
    x, c = f // 2, f % 2
    mate = f + 1 - 2 * c
    right, left = (b + 1) % nb, (b + nb - 1) % nb
    fright, fleft = (f + 2) % nf, (f + nf - 2) % nf
    lead = x + nx * c
    slot = (b - lead + nf // 2 + nb) % nb
    to_band = (b - nf // 2 + (SPREAD * f) % nf + nb) % nb
    to_fft = 2 * (b % nx) + (b // nx) % 2
    to_slot = (b // nf) * nf + f
    from_fft = (SPREAD * slot) % nf
    from_band = lead + nf * (slot // nf)
    alone = jnp.logical_and(to_band == b, to_fft == f)

    def farthest_first(i, count):
        return count // 2 + jnp.where(i % 2 == 0, i // 2, -(i // 2))

    def rows(start, count):
        return pl.ds(pl.multiple_of(start, 8), count)

    def rc(src, dst, ssem, rsem, **dev):
        return pltpu.make_async_remote_copy(
            src_ref=src, dst_ref=dst, send_sem=ssem, recv_sem=rsem, device_id=dev,
            device_id_type=MESH,
        )

    perm_s, agz_s, agx_s, du_s, dv_s, rs_s = [many.at[k] for k in range(6)]
    au_s, av_s, ap_s, mf_s, mb_s = [many.at[k] for k in range(6, 11)]
    au_r, av_r, ap_r, mf_r, mb_r = [many.at[k] for k in range(11, 16)]

    def all_sent(ref, sem):
        rc(ref, ref, sem, sem, fft=mate).wait_send()

    def all_here(ref, sem):
        rc(ref, ref, sem, sem, fft=mate).wait_recv()

    barrier = pltpu.get_barrier_semaphore()

    def greet(**dev):
        pl.semaphore_signal(barrier, inc=1, device_id=dev, device_id_type=MESH)

    greet(band=right)
    greet(band=left)
    greet(fft=fright)
    greet(fft=fleft)
    greet(fft=mate)

    @pl.when(jnp.logical_not(alone))
    def _():
        greet(band=to_band, fft=to_fft)
        greet(band=from_band, fft=from_fft)

    tables = [
        pltpu.make_async_copy(src, dst, loc.at[7 + k])
        for k, (src, dst) in enumerate(
            ((zf_hbm, zf_ref), (zi_hbm, zi_ref), (lf_hbm, lf_ref), (li_hbm, li_ref))
        )
    ]
    p_local = pltpu.make_async_copy(p_hbm, p_own, loc.at[11])
    p_local.start()
    for table in tables:
        table.start()
    u_local = pltpu.make_async_copy(u_hbm, ufull.at[rows(f * slab, slab)], loc.at[0])
    u_local.start()
    p_local.wait()
    pl.semaphore_wait(barrier, jnp.where(alone, 5, 7))

    def place(at):
        return (at // nf) * nf + (SPREAD * at) % nf

    def perm(q):
        return rc(
            p_own.at[rows(q * quarter, quarter)],
            pfull.at[rows(to_slot * slab + q * quarter, quarter)],
            perm_s, perm_r.at[q], band=to_band, fft=to_fft,
        )

    def perm_here(q):
        return rc(
            p_own.at[rows(q * quarter, quarter)],
            pfull.at[rows(place(slot) * slab + q * quarter, quarter)],
            perm_s, perm_r.at[q], band=from_band, fft=from_fft,
        )

    def perm_local(q):
        return pltpu.make_async_copy(
            p_hbm.at[rows(q * quarter, quarter)],
            pfull.at[rows(place(slot) * slab + q * quarter, quarter)], loc.at[2 + q],
        )

    @pl.when(jnp.logical_not(alone))
    def _():
        for q in range(quarters):
            perm(q).start()

    @pl.when(alone)
    def _():
        for q in range(quarters):
            perm_local(q).start()

    def slab_of(dx, core):
        return 2 * ((x + dx) % nx) + core

    def agx1(h, way):
        return rc(
            u_hbm.at[rows(h * half, half)], ufull.at[rows(f * slab + h * half, half)],
            agx_s, agx_r.at[0, h, way], fft=fright if way == 0 else fleft,
        )

    def agx1_here(h, way):
        owner = slab_of(nx - 1 if way == 0 else 1, c)
        return rc(
            u_hbm.at[rows(h * half, half)], ufull.at[rows(owner * slab + h * half, half)],
            agx_s, agx_r.at[0, h, way], fft=fright if way == 0 else fleft,
        )

    def agx2(way):
        owner = slab_of(nx - 1 if way == 0 else 1, c)
        piece = ufull.at[rows(owner * slab + way * half, half)]
        return rc(
            piece, piece, agx_s, agx_r.at[1, 0, way],
            fft=fright if way == 0 else fleft,
        )

    def agx2_here(way):
        piece = ufull.at[rows(slab_of(2, c) * slab + way * half, half)]
        return rc(
            piece, piece, agx_s, agx_r.at[1, 0, way],
            fft=fright if way == 0 else fleft,
        )

    def du(k, core):
        piece = ufull.at[rows(slab_of((0, nx - 1, 1, 2)[k], core) * slab, slab)]
        src = u_hbm if (k == 0) else piece
        return rc(src, piece, du_s, du_r.at[k], fft=mate)

    du(0, c).start()

    def agz(s, q, way):
        owner = (slot - (s - 1) + nb) % nb if way == 0 else (slot + (s - 1)) % nb
        piece = pfull.at[rows(place(owner) * slab + q * quarter, quarter)]
        return rc(
            piece, piece, agz_s, agz_r.at[s, q, way],
            band=right if way == 0 else left,
        )

    def agz_here(s, q, way):
        owner = (slot - s + nb) % nb if way == 0 else (slot + s) % nb
        piece = pfull.at[rows(place(owner) * slab + q * quarter, quarter)]
        return rc(
            piece, piece, agz_s, agz_r.at[s, q, way],
            band=right if way == 0 else left,
        )

    for q in range(quarters):
        @pl.when(jnp.logical_not(alone))
        def _():
            perm_here(q).wait_recv()

        @pl.when(alone)
        def _():
            perm_local(q).wait()

        for way in (0, 1):
            agz(1, q, way).start()

    for way in (0, 1):
        agx1(way, way).start()
    for way in (0, 1):
        agx1(1 - way, way).start()

    def forward(s, q):
        for way in (0, 1):
            agz_here(s - 1, q, way).wait_recv()
            agz(s, q, way).start()

    for q in range(quarters):
        forward(2, q)
    for way in (0, 1):
        agx1_here(way, way).wait_recv()
        agx2(way).start()
    for q in range(quarters):
        forward(3, q)
    for way in (0, 1):
        agx1_here(1 - way, way).wait_recv()
        du(1 + way, c).start()
    for q in range(quarters):
        forward(4, q)
    for way in (0, 1):
        agx2_here(way).wait_recv()
    du(3, c).start()
    u_local.wait()
    for table in tables:
        table.wait()
    for k in range(4):
        du(k, 1 - c).wait_recv()

    first_lanes = lax.broadcasted_iota(jnp.int32, (1, width), 1) < width // 2
    batch = 4

    def forward_planes(owner, k):
        a, s = owner // nf, owner % nf
        p = pfull[rows(owner * slab + k * batch * n, batch * n), :]
        u = ufull[rows(s * slab + k * batch * n, batch * n), :]
        ps, us = swapped(p), swapped(u)
        real = jnp.where(first_lanes, p, ps)
        imag = jnp.where(first_lanes, ps, -p)
        rho = real * u + imag * us
        spec = along_last(rho, zf_ref[...])
        base = (a * n + s * planes + k * batch) * pitch
        for q in range(0, batch, 2):
            outs = along_left(
                [spec[q * n : (q + 1) * n], spec[(q + 1) * n : (q + 2) * n]], lf_ref[...]
            )
            for e in (0, 1):
                dbuf[rows(base + (q + e) * pitch, n), :] = outs[e]

    last = nb // 2

    per_slab = planes // batch
    assert per_slab == 2 and quarters == 4

    def items_ready(t):
        q = t % quarters
        ready = 2 * (2 * (t // quarters + first - 2) + 1) + 2 * ((q + 1) // 2)
        return jnp.minimum(2 * (t + 1), ready)

    first = 5

    def items(start, stop):
        @pl.loop(start, stop)
        def _(w):
            far = (w + 2) // 4
            ends = jnp.logical_or(w < 2, w >= nb * per_slab - 2)
            k = jnp.where(ends, w % 2, (w - 2) // 2 % 2)
            owner = jnp.where(ends | (w % 2 == 0), slot + far, slot - far + nb) % nb
            forward_planes(place(owner), k)

    @pl.loop(0, quarters * (last + 1 - first))
    def _(t):
        s, q = first + t // quarters, t % quarters

        @pl.when(s < last)
        def _():
            forward(s, q)

        @pl.when(s == last)
        def _():
            for way in (0, 1):
                agz_here(s - 1, q, way).wait_recv()

                @pl.when(2 * q // quarters == way)
                def _():
                    agz(s, q, way).start()

        items(jnp.where(t == 0, 0, items_ready(t - 1)), items_ready(t))

    bit = part // 2

    def in_slab(t, h):
        return rows(h * half + t * bit, bit)

    def in_parts(t, h):
        return rows(t * part + h * bit, bit)

    def spread(src, dst, ssem, rsem, h, d):
        to = (b + d) % nb
        return rc(src.at[in_slab(to, h)], dst.at[in_parts(b, h)], ssem, rsem, band=to)

    def gather(h, d):
        to = (b + d) % nb
        return rc(psub.at[in_parts(to, h)], proj_ref.at[in_slab(b, h)], ap_s, ap_r, band=to)

    au = (u_hbm, usub, au_s, au_r)
    av = (pot_ref, vsub, av_s, av_r)

    def u_mine(h):
        return pltpu.make_async_copy(
            u_hbm.at[in_slab(b, h)], usub.at[in_parts(b, h)], loc.at[1 if h == 0 else 6]
        )

    freq = lax.broadcasted_iota(jnp.int32, (n, width), 0)
    freq = jnp.where(freq < n // 2, freq, freq - n).astype(F32)
    lane = lax.broadcasted_iota(jnp.int32, (n, width), 1) % n
    lane = jnp.where(lane < n // 2, lane, lane - n).astype(F32)
    scale = FOUR_PI / n**3
    per = 16
    done = items_ready(quarters * (last + 1 - first) - 1)
    before = (nb - 1) * per_slab

    def orbital_parts(start, stop):
        @pl.loop(start, stop, unroll=True)
        def _(i):
            for h in (0, 1):
                spread(*au, h, farthest_first(i, nb)).start()

    @pl.loop(0, 2)
    def _(m):
        @pl.when(m == 1)
        def _():
            for q in range(quarters):
                agz_here(last, q, 2 * q // quarters).wait_recv()
            orbital_parts(last, nb)

        items(jnp.where(m == 0, done, before), jnp.where(m == 0, before, nb * per_slab))
        a = (slot // nf + m) % 2
        row = idx_ref[lead + nf * a]
        qx, qy, qz = [tab_ref[e, row] for e in range(3)]
        fx, fz = freq + qx, lane + qz
        hops[pl.ds(0, n), :] = fx * fx + fz * fz + SCREEN_SQUARE

        @pl.loop(0, n // per)
        def _(k):
            taken, spectra = [], []
            for y in range(0, per, 2):
                take = [pl.ds(a * n * pitch + k * per + y + e, n, stride=pitch) for e in (0, 1)]
                taken.append(take)
                spectra.append(along_left([dbuf[t, :] for t in take], lf_ref[...]))
            base = hops[pl.ds(0, n), :]
            screened = []
            for y, pair in zip(range(0, per, 2), spectra):
                both = []
                for e in (0, 1):
                    at = k * per + y + e
                    fy = jnp.where(at < n // 2, at, at - n).astype(F32) + qy
                    both.append(pair[e] * (scale / (base + fy * fy)))
                screened.append(both)
            for take, both in zip(taken, screened):
                for t, field in zip(take, along_left(both, li_ref[...])):
                    dbuf[t, :] = field

    order = (2, 1, nx - 1, 0)

    orbital_parts(1, last)
    for h in (0, 1):
        u_mine(h).start()

    def dv(h, k):
        src = vbuf.at[rows(slab_of(order[k], 1 - c) * slab + h * half, half)]
        return rc(
            src, d2d.at[rows(k * slab + h * half, half)], dv_s, dv_r.at[h, k], fft=mate
        )

    def landing(h, k):
        return rows(2 * n + (h * 6 + k) * quarter, quarter)

    def own_rows(dx, h, e):
        return rows(slab_of(dx, c) * slab + h * half + e * quarter, quarter)

    def hop(h, k):
        way = k % 2
        toward = 1 if way == 0 else nx - 1
        piece = own_rows(2 if k < 2 else toward, h, 1 - way if k in (2, 3) else way)
        return rc(
            vbuf.at[piece], hops.at[landing(h, k)], rs_s, rs_r.at[h, k],
            fft=fright if way == 0 else fleft,
        )

    def inverse_halves(h, pair, core):
        at = [slab_of(order[k], core) for k in pair]
        total = None
        for a in (0, 1):
            fields = []
            for s in at:
                base = (a * n + s * planes + h * (planes // 2)) * pitch
                for e in range(0, planes // 2, 2):
                    fields += along_left(
                        [dbuf[rows(base + (e + g) * pitch, n), :] for g in (0, 1)], li_ref[...]
                    )
            field = along_last(jnp.concatenate(fields, axis=0), zi_ref[...])
            p = jnp.concatenate(
                [pfull[rows((a * nf + s) * slab + h * half, half), :] for s in at], axis=0
            )
            ps = swapped(p)
            real = jnp.where(first_lanes, p, ps)
            imag = jnp.where(first_lanes, -ps, p)
            term = real * field + imag * swapped(field)
            total = term if total is None else total + term
        for k, s in enumerate(at):
            vbuf[rows(s * slab + h * half, half), :] = total[k * half : (k + 1) * half]

    def relay(h):
        for way in (0, 1):
            hop(h, way).wait_recv()
            toward = own_rows(1 if way == 0 else nx - 1, h, way)
            vbuf[toward, :] += hops[landing(h, way), :]
            hop(h, 4 + way).start()

    def with_mate(h, k):
        dv(h, k).wait_recv()
        own = rows(slab_of(order[k], c) * slab + h * half, half)
        vbuf[own, :] += d2d[rows(k * slab + h * half, half), :]

    @pl.loop(0, 2)
    def _(h):
        inverse_halves(h, (0, 1), 1 - c)
        dv(h, 0).start()
        dv(h, 1).start()
        inverse_halves(h, (0, 1), c)
        inverse_halves(h, (2, 3), 1 - c)
        dv(h, 2).start()
        dv(h, 3).start()

        @pl.when(h == 1)
        def _():
            relay(0)

        with_mate(h, 0)
        hop(h, 0).start()
        hop(h, 1).start()
        with_mate(h, 1)
        hop(h, 2).start()
        inverse_halves(h, (2, 3), c)
        with_mate(h, 2)
        hop(h, 3).start()
        with_mate(h, 3)

    for h in (0, 1):
        if h == 1:
            relay(1)
        for k in (2, 3, 4, 5):
            hop(h, k).wait_recv()
        pot_ref[rows(h * half, quarter), :] = (
            vbuf[own_rows(0, h, 0), :] + hops[landing(h, 3), :] + hops[landing(h, 4), :]
        )
        pot_ref[rows(h * half + quarter, quarter), :] = (
            vbuf[own_rows(0, h, 1), :] + hops[landing(h, 2), :] + hops[landing(h, 5), :]
        )

        @pl.loop(1, nb, unroll=True)
        def _(m):
            spread(*av, h, farthest_first(m, nb)).start()

    for h in (0, 1):
        vsub[in_parts(b, h), :] = pot_ref[in_slab(b, h), :]
        u_mine(h).wait()

    others = pl.ds(0, (nb - 1) * part)
    all_here(usub.at[others], au_r)
    all_here(vsub.at[others], av_r)

    group = 4
    acc = jnp.zeros((2 * nb, 4 * nb), F32)
    for g in range(0, part, group):
        us = [usub[pl.ds(g + e, nb, stride=part), :] for e in range(group)]
        vs = [vsub[pl.ds(g + e, nb, stride=part), :] for e in range(group)]
        uh, ul = halves(jnp.concatenate(us, axis=1))
        vh, vl = halves(jnp.concatenate(vs, axis=1))
        th, tl = halves(jnp.concatenate([turned(v) for v in vs], axis=1))
        acc += lax.dot_general(
            jnp.concatenate([uh, ul], axis=0), jnp.concatenate([vh, th, vl, tl], axis=0),
            (((1,), (1,)), ((), ())), preferred_element_type=F32,
        )
    acc = acc[:nb] + acc[nb:]
    acc = (acc[:, : 2 * nb] + acc[:, 2 * nb :]) * (1.0 / n**3)
    folds = width // (2 * nb)
    tall = nb // folds
    mine[...] = jnp.concatenate([acc[k * tall : (k + 1) * tall] for k in range(folds)], axis=1)

    def mf(d):
        to = (f + d) % nf
        return rc(mine, mrow.at[f], mf_s, mf_r, fft=to)

    def mb(d):
        to = (b + d) % nb
        return rc(mcol, mall.at[b], mb_s, mb_r, band=to)

    for i in range(1, nf):
        mf(nf // 2 + (i // 2 if i % 2 == 0 else -(i // 2))).start()
    mrow[f] = mine[...]
    all_here(mrow.at[pl.ds(0, nf - 1)], mf_r)
    total = mrow[0]
    for k in range(1, nf):
        total += mrow[k]
    mcol[...] = total

    @pl.loop(1, nb)
    def _(i):
        mb(farthest_first(i, nb)).start()

    mall[b] = mcol[...]

    all_here(mall.at[pl.ds(0, nb - 1)], mb_r)

    total = mall[0]
    for k in range(1, nb):
        total += mall[k]
    total = jnp.concatenate(
        [total[:, 2 * nb * k : 2 * nb * (k + 1)] for k in range(folds)], axis=0
    )

    ri = lax.broadcasted_iota(jnp.int32, (nb, nb), 0)
    ci = lax.broadcasted_iota(jnp.int32, (nb, nb), 1)
    eye = (ri == ci).astype(F32)

    def flipped(m):
        return lax.dot_general(
            eye, m, (((1,), (1,)), ((), ())), precision=lax.Precision.HIGHEST,
            preferred_element_type=F32,
        )

    mre, mim = total[:, :nb], total[:, nb : 2 * nb]
    hre = jnp.where(ri >= ci, mre, flipped(mre))
    him = jnp.where(ri > ci, mim, jnp.where(ri < ci, -flipped(mim), 0.0))
    zero = jnp.zeros((nb, nb), F32)
    work = jnp.concatenate([hre, him, eye, zero], axis=1)
    other = jnp.concatenate([-him, hre, zero, eye], axis=1)
    below = lax.broadcasted_iota(jnp.int32, work.shape, 0)
    for k in range(nb):
        inverse = 1.0 / jnp.broadcast_to(work[k : k + 1, k : k + 1], (1, 4 * nb))
        row, rot = work[k : k + 1, :] * inverse, other[k : k + 1, :] * inverse
        cre = jnp.where(below > k, jnp.broadcast_to(work[:, k : k + 1], work.shape), 0.0)
        cim = jnp.where(
            below > k, jnp.broadcast_to(work[:, nb + k : nb + k + 1], work.shape), 0.0
        )
        work = work - (cre * row + cim * rot)
        other = other - (cre * rot - cim * row)
    pivots = jnp.sum(work[:, :nb] * eye, axis=1, keepdims=True)
    coef = work[:, 2 * nb : 4 * nb] / jnp.sqrt(pivots)
    ch, cl = halves(coef)
    coef = jnp.concatenate(
        [jnp.concatenate([ch, ch], axis=1), jnp.concatenate([cl, cl], axis=1)], axis=0
    )

    for g in range(0, part, group):
        vs = [vsub[pl.ds(g + e, nb, stride=part), :] for e in range(group)]
        cols = jnp.concatenate([left_column(v) for v in vs], axis=1)
        both = mm(coef, cols)
        out = both[:nb] + both[nb:]
        for e in range(group):
            psub[pl.ds(g + e, nb, stride=part), :] = out[:, e * width : (e + 1) * width]

    @pl.loop(1, nb)
    def _(i):
        for h in (0, 1):
            gather(h, farthest_first(i, nb)).start()

    for h in (0, 1):
        proj_ref[in_slab(b, h), :] = psub[in_parts(b, h), :]

    @pl.when(jnp.logical_not(alone))
    def _():
        all_sent(pfull.at[pl.ds(0, slab)], perm_s)

    all_sent(pfull.at[pl.ds(0, (nb - 1) * slab)], agz_s)
    all_sent(ufull.at[pl.ds(0, (nx - 1) * slab)], agx_s)
    all_sent(ufull.at[pl.ds(0, nx * slab)], du_s)
    all_sent(vbuf.at[pl.ds(0, nx * slab)], dv_s)
    all_sent(vbuf.at[pl.ds(0, (nx - 1) * slab)], rs_s)
    all_sent(usub.at[others], au_s)
    all_sent(vsub.at[others], av_s)
    all_sent(mrow.at[pl.ds(0, nf - 1)], mf_s)
    all_sent(mall.at[pl.ds(0, nb - 1)], mb_s)
    all_sent(psub.at[others], ap_s)
    all_here(proj_ref.at[others], ap_r)


def body(mesh, orbitals, partners, shift_table, shift_index):
    nb, nf = mesh.shape["band"], mesh.shape["fft"]
    n = orbitals.shape[2]
    width = orbitals.shape[3]
    slab = orbitals.shape[0] * orbitals.shape[1] * n
    part = slab // nb
    assert nb == 2 * nf and nf == 8 and SPREAD**2 % nf == 1 and orbitals.shape[0] == 1

    def call(p, u, *rest):
        any_spec = pl.BlockSpec(memory_space=pl.ANY)
        vmem = pl.BlockSpec(memory_space=pltpu.VMEM)
        smem = pl.BlockSpec(memory_space=pltpu.SMEM)
        dma = pltpu.SemaphoreType.DMA
        out = pltpu.VMEM((slab, width), F32)
        half = slab // 2
        tall = 2 * nb * nb // width
        return pl.pallas_call(
            lambda *refs: kernel(nb, nf, n, *refs),
            out_shape=(out, out),
            in_specs=[any_spec] * 6 + [smem, smem],
            out_specs=(vmem, vmem),
            scratch_shapes=[pltpu.VMEM(t.shape, BF) for t in rest[:4]] + [
                pltpu.VMEM((slab, width), F32),
                pltpu.VMEM((nb * slab, width), F32),
                pltpu.VMEM((nf * slab, width), F32),
                pltpu.VMEM((2 * n * (n + PAD), width), F32),
                pltpu.VMEM((nf * slab, width), F32),
                pltpu.VMEM((nf // 2 * slab, width), F32),
                pltpu.VMEM((2 * n + 6 * half, width), F32),
                pltpu.VMEM((slab, width), F32),
                pltpu.VMEM((slab, width), F32),
                pltpu.VMEM((slab, width), F32),
                pltpu.VMEM((tall, width), F32),
                pltpu.VMEM((nf, tall, width), F32),
                pltpu.VMEM((tall, width), F32),
                pltpu.VMEM((nb, tall, width), F32),
                dma((4,)), dma((12,)), dma((nb // 2 + 1, 4, 2)), dma((2, 2, 2)), dma((4,)),
                dma((2, 4)), dma((2, 6)), dma((16,)),
            ],
            compiler_params=pltpu.CompilerParams(collective_id=0, has_side_effects=True),
            name="exchange",
        )(p, u, *rest)

    tables = [
        jnp.asarray(t)
        for t in (last_table(n, -1.0), last_table(n, 1.0), left_table(n, -1.0), left_table(n, 1.0))
    ]
    pot, proj = call(
        partners.reshape(slab, width), orbitals.reshape(slab, width), *tables,
        shift_table.T, shift_index,
    )
    return pot.reshape(orbitals.shape), proj.reshape(orbitals.shape)


def solution(mesh):
    spec = P(("kgrp", "band"), "fft", None, None)
    return jax.shard_map(
        lambda *args: body(mesh, *args), mesh=mesh, in_specs=(spec, spec, P(), P("kgrp")),
        out_specs=(spec, spec), check_vma=False,
    )
```
